32 devices in a mesh: dp: 1 (over z), ep: 32 (over y, x, core).
Axes of the slice: x: 4, y: 4, z: 1, core: 2. Of those that a mesh axis runs over, the one named last changes fastest.
The devices are a block of a 4x4x8 slice.
Arguments:
- dy_home: bfloat16 [8192, 1024], P(('dp', 'ep'))
- topk_idx: int32 [8192, 8], P(('dp', 'ep'))
- slot_idx: int32 [8192, 8], P(('dp', 'ep'))
- gates: float32 [8192, 8], P(('dp', 'ep'))
- y_back: bfloat16 [8192, 8, 1024], P(('dp', 'ep'))
- x_disp: bfloat16 [32, 4096, 1024], P(('dp', 'ep'))
- h1_disp: bfloat16 [32, 4096, 512], P(('dp', 'ep'))
- h3_disp: bfloat16 [32, 4096, 512], P(('dp', 'ep'))
- w_gate: bfloat16 [32, 1024, 512], P('ep')
- w_up: bfloat16 [32, 1024, 512], P('ep')
- w_down: bfloat16 [32, 512, 1024], P('ep')
Outputs:
- output 1: bfloat16 [8192, 1024], P(('dp', 'ep'))
- output 2: float32 [8192, 8], P(('dp', 'ep'))
- output 3: float32 [32, 1024, 512], P(('dp', 'ep'))
- output 4: float32 [32, 1024, 512], P(('dp', 'ep'))
- output 5: float32 [32, 512, 1024], P(('dp', 'ep'))
All inputs are finite; a program needn't handle non-finite values.
Results may differ from the reference program's by a relative error of at most 0.0135394.
Values are sent between devices in bfloat16 or wider.
A program may use at most 768 MiB of HBM per device.

```python
import jax
import jax.numpy as jnp
from jax import lax

EP_SIZE = 32
TOKENS_DEV = 256
TOP = 8
EXPERTS = 32
D = 1024
FF = 512

CAPACITY = 2 * TOKENS_DEV * TOP // EXPERTS
ALL_TOKENS = EP_SIZE * TOKENS_DEV
ROWS_ALL = EXPERTS * EP_SIZE * CAPACITY


def rank_in_buffer(expert_ids):
    num_items = TOKENS_DEV * TOP
    positions = jnp.arange(num_items, dtype=jnp.int32)
    sort_order = jnp.argsort(expert_ids * num_items + positions)
    sorted_ids = expert_ids[sort_order]
    first_pos = jnp.searchsorted(sorted_ids, sorted_ids, side='left').astype(jnp.int32)
    buf_rank = jnp.zeros((num_items,), jnp.int32).at[sort_order].set(positions - first_pos)
    return jnp.where(buf_rank < CAPACITY, buf_rank, -1)


def route_draw(route_key):
    key_base, key_bias, key_hot = jax.random.split(route_key, 3)
    base_score = jax.random.randint(key_base, (ALL_TOKENS, EXPERTS), 0, 65536)
    expert_bias = jax.random.randint(key_bias, (EXPERTS,), 0, 32768)
    hot_expert = jax.random.randint(key_hot, (), 0, EXPERTS)
    tok_pos = jnp.arange(ALL_TOKENS, dtype=jnp.int32) % TOKENS_DEV
    expert_ids = jnp.arange(EXPERTS, dtype=jnp.int32)
    forced = (tok_pos[:, None] <= CAPACITY) & (expert_ids[None, :] == hot_expert)
    full_score = (base_score + expert_bias[None, :] + jnp.where(forced, 131072, 0)) * EXPERTS + expert_ids[None, :]
    topk_idx = lax.top_k(full_score, TOP)[1].astype(jnp.int32)
    slot_idx = jax.vmap(rank_in_buffer)(topk_idx.reshape(EP_SIZE, TOKENS_DEV * TOP))
    return topk_idx, slot_idx.reshape(ALL_TOKENS, TOP)


def buffer_index(topk_idx, slot_idx):
    src_dev = jnp.arange(ALL_TOKENS, dtype=jnp.int32) // TOKENS_DEV
    flat_pos = (topk_idx * EP_SIZE + src_dev[:, None]) * CAPACITY + slot_idx
    return jnp.where(slot_idx >= 0, flat_pos, ROWS_ALL)


def expert_forward(operands):
    x_expert, gate_w, up_w, down_w = operands
    h_gate = jnp.dot(x_expert, gate_w, preferred_element_type=jnp.float32).astype(jnp.bfloat16)
    h_up = jnp.dot(x_expert, up_w, preferred_element_type=jnp.float32).astype(jnp.bfloat16)
    hidden_act = (jax.nn.silu(h_gate.astype(jnp.float32)) * h_up.astype(jnp.float32)).astype(jnp.bfloat16)
    y_expert = jnp.dot(hidden_act, down_w, preferred_element_type=jnp.float32).astype(jnp.bfloat16)
    return h_gate, h_up, y_expert


def forward_buffers(x_tok, flat_pos, w_gate, w_up, w_down):
    x_rows = jnp.broadcast_to(x_tok[:, None, :], (ALL_TOKENS, TOP, D)).reshape(ALL_TOKENS * TOP, D)
    x_disp = jnp.zeros((ROWS_ALL, D), jnp.bfloat16).at[flat_pos.reshape(-1)].set(x_rows, mode='drop')
    x_disp = x_disp.reshape(EXPERTS, EP_SIZE * CAPACITY, D)
    h1_disp, h3_disp, y_disp = lax.map(expert_forward, (x_disp, w_gate, w_up, w_down))
    y_back = jnp.take(y_disp.reshape(ROWS_ALL, D), flat_pos, axis=0, mode='fill', fill_value=0)
    return y_back, x_disp, h1_disp, h3_disp


def setup_inputs(seed: int = 0, part: int = 0) -> dict:
    root_key = jax.random.key(seed)
    key_gate, key_up, key_down = jax.random.split(root_key, 3)
    w_gate = (jax.random.normal(key_gate, (EXPERTS, D, FF), jnp.float32) * D ** -0.5).astype(jnp.bfloat16)
    w_up = (jax.random.normal(key_up, (EXPERTS, D, FF), jnp.float32) * D ** -0.5).astype(jnp.bfloat16)
    w_down = (jax.random.normal(key_down, (EXPERTS, FF, D), jnp.float32) * FF ** -0.5).astype(jnp.bfloat16)
    part_key = jax.random.fold_in(root_key, part)
    key_route, key_tok, key_grad, key_mix = jax.random.split(part_key, 4)
    topk_idx, slot_idx = route_draw(key_route)
    gates = jax.random.uniform(key_mix, (ALL_TOKENS, TOP), jnp.float32, 0.2, 1.0)
    x_tok = jax.random.normal(key_tok, (ALL_TOKENS, D), jnp.float32).astype(jnp.bfloat16)
    dy_home = jax.random.normal(key_grad, (ALL_TOKENS, D), jnp.float32).astype(jnp.bfloat16)
    flat_pos = buffer_index(topk_idx, slot_idx)
    y_back, x_disp, h1_disp, h3_disp = forward_buffers(x_tok, flat_pos, w_gate, w_up, w_down)
    return {'dy_home': dy_home, 'topk_idx': topk_idx, 'slot_idx': slot_idx, 'gates': gates,
            'y_back': y_back, 'x_disp': x_disp, 'h1_disp': h1_disp, 'h3_disp': h3_disp,
            'w_gate': w_gate, 'w_up': w_up, 'w_down': w_down}


def expert_backward(operands):
    dy_expert, x_expert, h_gate, h_up, gate_w, up_w, down_w = operands
    gate_f = h_gate.astype(jnp.float32)
    up_f = h_up.astype(jnp.float32)
    sig_gate = jax.nn.sigmoid(gate_f)
    silu_g = gate_f * sig_gate
    hidden_act = (silu_g * up_f).astype(jnp.bfloat16)
    d_act = jnp.dot(dy_expert, down_w.T, preferred_element_type=jnp.float32).astype(jnp.bfloat16).astype(jnp.float32)
    dh_gate = (d_act * up_f * sig_gate * (1.0 + gate_f * (1.0 - sig_gate))).astype(jnp.bfloat16)
    dh_up = (d_act * silu_g).astype(jnp.bfloat16)
    dw_down = jnp.dot(hidden_act.T, dy_expert, preferred_element_type=jnp.float32)
    dw_gate = jnp.dot(x_expert.T, dh_gate, preferred_element_type=jnp.float32)
    dw_up = jnp.dot(x_expert.T, dh_up, preferred_element_type=jnp.float32)
    dx_expert = (jnp.dot(dh_gate, gate_w.T, preferred_element_type=jnp.float32)
                 + jnp.dot(dh_up, up_w.T, preferred_element_type=jnp.float32)).astype(jnp.bfloat16)
    return dx_expert, dw_gate, dw_up, dw_down


def reference(dy_home, topk_idx, slot_idx, gates, y_back, x_disp, h1_disp, h3_disp, w_gate, w_up, w_down):
    d_gates = jnp.einsum('td,tjd->tj', dy_home.astype(jnp.float32), y_back.astype(jnp.float32))
    flat_pos = buffer_index(topk_idx, slot_idx)
    gated_rows = (gates[:, :, None] * dy_home[:, None, :].astype(jnp.float32)).astype(jnp.bfloat16)
    dy_disp = jnp.zeros((ROWS_ALL, D), jnp.bfloat16).at[flat_pos.reshape(-1)].set(gated_rows.reshape(ALL_TOKENS * TOP, D), mode='drop')
    dy_disp = dy_disp.reshape(EXPERTS, EP_SIZE * CAPACITY, D)
    dx_disp, dw_gate, dw_up, dw_down = lax.map(expert_backward, (dy_disp, x_disp, h1_disp, h3_disp, w_gate, w_up, w_down))
    returned = jnp.take(dx_disp.reshape(ROWS_ALL, D), flat_pos, axis=0, mode='fill', fill_value=0)
    dx_home = jnp.sum(returned.astype(jnp.float32), axis=1).astype(jnp.bfloat16)
    return dx_home, d_gates, dw_gate, dw_up, dw_down
```

```python
import functools

import jax
import jax.numpy as jnp
from jax import lax
from jax.experimental import pallas as pl
from jax.experimental.pallas import tpu as pltpu
from jax.sharding import PartitionSpec as P

F32 = jnp.float32
BF16 = jnp.bfloat16


def mm(a, b, dims):
    return lax.dot_general(a, b, (dims, ((), ())), preferred_element_type=F32)


def gated_rows(dy, slot, gate, capacity):
    rows = lax.broadcasted_iota(jnp.int32, (capacity, slot.shape[1]), 0).astype(F32)
    hit = rows == slot
    row_gate = jnp.sum(jnp.where(hit, gate, 0.0), axis=1, keepdims=True)
    picked = mm(jnp.where(hit, 1.0, 0.0).astype(BF16), dy, ((1,), (0,)))
    return (row_gate * picked).astype(BF16)


def expert_kernel(dy_ref, tab_ref, x_ref, h1_ref, h3_ref, w1_ref, w3_ref, w2_ref,
                  dx_ref, dw1_ref, dw3_ref, dw2_ref, dyd_ref, dh_ref):
    capacity = dx_ref.shape[0] // dy_ref.shape[0]
    ff = h1_ref.shape[1]

    @pl.when(pl.program_id(0) == 0)
    def _():
        dw1_ref[...] = jnp.zeros_like(dw1_ref)
        dw3_ref[...] = jnp.zeros_like(dw3_ref)
        dw2_ref[...] = jnp.zeros_like(dw2_ref)

    for i in range(dy_ref.shape[0]):
        dyd_ref[i * capacity:(i + 1) * capacity, :] = gated_rows(
            dy_ref[i], tab_ref[i, 0:1, :], tab_ref[i, 1:2, :], capacity)
    dyd = dyd_ref[...]
    d_act = mm(dyd, w2_ref[...], ((1,), (1,))).astype(BF16).astype(F32)
    g = h1_ref[...].astype(F32)
    u = h3_ref[...].astype(F32)
    sg = jax.nn.sigmoid(g)
    silu = g * sg
    act = (silu * u).astype(BF16)
    dh_ref[:, 0:ff] = (d_act * u * sg * (1.0 + g * (1.0 - sg))).astype(BF16)
    dh_ref[:, ff:2 * ff] = (d_act * silu).astype(BF16)
    dw2_ref[...] += mm(act, dyd, ((0,), (0,)))
    dh1 = dh_ref[:, 0:ff]
    dh3 = dh_ref[:, ff:2 * ff]
    dw1_ref[...] += mm(x_ref[...], dh1, ((0,), (0,)))
    dw3_ref[...] += mm(x_ref[...], dh3, ((0,), (0,)))
    dx_ref[...] = (mm(dh1, w1_ref[...], ((1,), (1,))) + mm(dh3, w3_ref[...], ((1,), (1,)))).astype(BF16)


def combine_kernel(slot_ref, rows_ref, dx_ref, acc_ref):
    capacity = rows_ref.shape[1]
    step = pl.program_id(0)

    @pl.when(step == 0)
    def _():
        acc_ref[...] = jnp.zeros_like(acc_ref)

    rows = lax.broadcasted_iota(jnp.int32, (capacity, slot_ref.shape[2]), 0).astype(F32)
    for i in range(rows_ref.shape[0]):
        hit = jnp.where(rows == slot_ref[i], 1.0, 0.0).astype(BF16)
        acc_ref[...] += mm(hit, rows_ref[i], ((0,), (0,)))

    @pl.when(step == pl.num_programs(0) - 1)
    def _():
        dx_ref[...] = acc_ref[...].astype(BF16)


def dgates_kernel(dy_ref, yb_ref, out_ref):
    out_ref[...] = jnp.sum(dy_ref[...].astype(F32)[:, None, :] * yb_ref[...].astype(F32), axis=2)


def solution(mesh):
    ep_size = mesh.shape['ep']
    tok_spec = P(('dp', 'ep'), None)
    buf_spec = P(('dp', 'ep'), None, None)
    expert_spec = P('ep', None, None)

    def device_step(dy, topk_idx, slot_idx, gates, y_back, x_disp, h1_disp, h3_disp, w_gate, w_up, w_down):
        capacity = x_disp.shape[1] // ep_size
        tokens, d = dy.shape
        top = gates.shape[1]
        ff = w_gate.shape[2]
        num_experts = w_gate.shape[0] * ep_size
        pair = 2
        rows = pair * capacity

        hit = topk_idx[None, :, :] == jnp.arange(num_experts, dtype=jnp.int32)[:, None, None]
        slot_of = (jnp.sum(jnp.where(hit, slot_idx[None] + 1, 0), axis=2) - 1).astype(F32)
        gate_of = jnp.sum(jnp.where(hit, gates[None], 0.0), axis=2)
        tab = lax.all_to_all(jnp.stack([slot_of, gate_of], axis=1), 'ep', 0, 0, tiled=True)
        dy_all = lax.all_gather(dy, 'ep', axis=0, tiled=False)

        params = pltpu.CompilerParams(vmem_limit_bytes=56 * 2 ** 20)
        tb = 32
        d_gates = pl.pallas_call(
            dgates_kernel, grid=(tokens // tb,),
            in_specs=[pl.BlockSpec((tb, d), lambda i: (i, 0)), pl.BlockSpec((tb, top, d), lambda i: (i, 0, 0))],
            out_specs=pl.BlockSpec((tb, top), lambda i: (i, 0)),
            out_shape=jax.ShapeDtypeStruct((tokens, top), F32), name='dgates',
            cost_estimate=pl.CostEstimate(flops=2 * tokens * top * d, bytes_accessed=2 * tokens * top * d, transcendentals=0),
        )(dy, y_back)

        const = lambda *shape: pl.BlockSpec(shape, lambda i: (0,) * len(shape))
        dx_rows, dw1, dw3, dw2 = pl.pallas_call(
            expert_kernel, grid=(ep_size // pair,),
            in_specs=[pl.BlockSpec((pair, tokens, d), lambda i: (i, 0, 0)),
                      pl.BlockSpec((pair, 2, tokens), lambda i: (i, 0, 0)),
                      pl.BlockSpec((rows, d), lambda i: (i, 0)),
                      pl.BlockSpec((rows, ff), lambda i: (i, 0)),
                      pl.BlockSpec((rows, ff), lambda i: (i, 0)),
                      const(d, ff), const(d, ff), const(ff, d)],
            out_specs=[pl.BlockSpec((rows, d), lambda i: (i, 0)), const(d, ff), const(d, ff), const(ff, d)],
            out_shape=[jax.ShapeDtypeStruct((ep_size * capacity, d), BF16),
                       jax.ShapeDtypeStruct((d, ff), F32), jax.ShapeDtypeStruct((d, ff), F32),
                       jax.ShapeDtypeStruct((ff, d), F32)],
            scratch_shapes=[pltpu.VMEM((rows, d), BF16), pltpu.VMEM((rows, 2 * ff), BF16)],
            compiler_params=params, name='experts',
        )(dy_all, tab, x_disp[0], h1_disp[0], h3_disp[0], w_gate[0], w_up[0], w_down[0])

        back = lax.all_to_all(dx_rows.reshape(ep_size, capacity, d), 'ep', 0, 0, tiled=True)
        eb = 4
        dx = pl.pallas_call(
            combine_kernel, grid=(num_experts // eb,),
            in_specs=[pl.BlockSpec((eb, 1, tokens), lambda i: (i, 0, 0)),
                      pl.BlockSpec((eb, capacity, d), lambda i: (i, 0, 0))],
            out_specs=const(tokens, d),
            out_shape=jax.ShapeDtypeStruct((tokens, d), BF16),
            scratch_shapes=[pltpu.VMEM((tokens, d), F32)],
            compiler_params=params, name='combine',
        )(slot_of[:, None, :], back)
        return dx, d_gates, dw1[None], dw3[None], dw2[None]

    return jax.shard_map(
        device_step, mesh=mesh,
        in_specs=(tok_spec, tok_spec, tok_spec, tok_spec, buf_spec, buf_spec, buf_spec, buf_spec,
                  expert_spec, expert_spec, expert_spec),
        out_specs=(tok_spec, tok_spec, buf_spec, buf_spec, buf_spec),
        check_vma=False)
```

```python
import functools
import math

import jax
import jax.numpy as jnp
from jax import lax
from jax.experimental import pallas as pl
from jax.experimental.pallas import tpu as pltpu
from jax.sharding import PartitionSpec as P

F32 = jnp.float32
BF16 = jnp.bfloat16

ORDER = ((2, 2), (2, 1), (1, 2), (2, 3), (3, 2), (2, 0), (0, 2),
         (1, 1), (1, 3), (3, 1), (1, 0), (0, 1), (3, 3), (3, 0), (0, 3), (0, 0))
SUMS = ((8, 1, 2), (9, 0, 2), (13, 1, 1), (14, 0, 1), (16, 1, 3), (17, 0, 3), (18, 1, 0), (19, 0, 0))
RELAY_LAG = 2
SUM_RELAYS = ((12, 1), (13, 0))
STEPS = 20


def mm(a, b, dims):
    return lax.dot_general(a, b, (dims, ((), ())), preferred_element_type=F32)


def pick(k, values):
    out = jnp.int32(values[0])
    for i, v in enumerate(values[1:], 1):
        out = jnp.where(k == i, jnp.int32(v), out)
    return out


def kernel_body(side, capacity, dy_ref, tab_in, x_ref, h1_ref, h3_ref, w1_ref, w3_ref, w2_ref,
                dx_ref, dw1_ref, dw3_ref, dw2_ref,
                dyall, tab, w1, w3, w2, dw1, dw3, dw2, xb, h1b, h3b, dyd, dh, dxs, rcv, hitb,
                psend, pown, precv, prelay,
                load_sem, w_sem, in_sem, out_sem, ag_send, ag_recv, ag_recv2, tb_send, tb_recv, tb_recv2,
                r_send, r_recv, rl_send, p_send, p_recv, pl_send, pl_recv):
    tokens = dyall.shape[2]
    top = tab.shape[1] // 2
    half = dyall.shape[3]
    ff = h1b.shape[2]
    rows = 2 * capacity
    piece = tokens // 2
    row_len = 2 * side
    me = lax.axis_index('ep')
    core = me % 2
    x = (me // 2) % side
    y = me // (2 * side)
    far = side // 2

    def wrap(v):
        return (v + side) % side

    def block(bx, by):
        return by * side + bx

    def device(bx, by, c):
        return {'ep': block(bx, by) * 2 + c}

    def chip(f, r1, r2):
        return (wrap(x + r1), wrap(y + r2)) if f == 0 else (wrap(x + r2), wrap(y + r1))

    loads = [pltpu.make_async_copy(dy_ref.at[:, pl.ds(f * half, half)], dyall.at[me, f], load_sem.at[f]) for f in (0, 1)]
    loads.append(pltpu.make_async_copy(tab_in, tab.at[me], load_sem.at[2]))
    wloads = [pltpu.make_async_copy(a, b, w_sem.at[i]) for i, (a, b) in enumerate(((w1_ref, w1), (w3_ref, w3), (w2_ref, w2)))]
    for cp in loads + wloads:
        cp.start()

    def stream(k):
        b = block(wrap(x + pick(k, [o[0] for o in ORDER])), wrap(y + pick(k, [o[1] for o in ORDER])))
        s = k % 2
        src = pl.ds(b * rows, rows)
        return [pltpu.make_async_copy(x_ref.at[src], xb.at[s], in_sem.at[s, 0]),
                pltpu.make_async_copy(h1_ref.at[src], h1b.at[s], in_sem.at[s, 1]),
                pltpu.make_async_copy(h3_ref.at[src], h3b.at[s], in_sem.at[s, 2])]

    for cp in stream(jnp.int32(0)):
        cp.start()

    barrier = pltpu.get_barrier_semaphore()
    for c in (0, 1):
        for bx, by in ((wrap(x + 1), y), (wrap(x - 1), y), (x, wrap(y + 1)), (x, wrap(y - 1))):
            pl.semaphore_signal(barrier, inc=1, device_id=device(bx, by, c))
    pl.semaphore_signal(barrier, inc=1, device_id=device(x, y, 1 - core))
    pl.semaphore_wait(barrier, 9)

    def gather_copy(f, p, r1, r2, axis, sign):
        bx, by = chip(f, r1, r2)
        home = block(bx, by) * 2 + core
        src = dyall.at[home, f, pl.ds(p * piece, piece)]
        if axis is None:
            dev, rs, ts = device(x, y, 1 - core), ag_recv2, tb_recv2
        else:
            nx, ny = chip(f, sign, 0) if axis == 0 else chip(f, 0, sign)
            dev, rs, ts = device(nx, ny, core), ag_recv, tb_recv
        out = [pltpu.make_async_remote_copy(src, src, ag_send, rs.at[block(bx, by), f, p], device_id=dev)]
        if f == 0:
            t = tab.at[home, pl.ds(p * top, top)]
            out.append(pltpu.make_async_remote_copy(t, t, tb_send, ts.at[block(bx, by), p], device_id=dev))
        return out

    def send(f, p, r1, r2, axis, sign=0):
        for cp in gather_copy(f, p, r1, r2, axis, sign):
            cp.start()

    def arrived(f, p, r1, r2):
        for cp in gather_copy(f, p, r1, r2, 0, 1):
            cp.wait_recv()

    for cp in loads:
        cp.wait()
    for axis in (0, 1):
        for f in (0, 1):
            for p, sign in ((0, 1), (1, -1), (1, 1), (0, -1)):
                send(f, p, 0, 0, axis, sign)
    for f in (0, 1):
        for p in (0, 1):
            send(f, p, 0, 0, None)

    def second_axis(f, p, r1):
        send(f, p, r1, 0, 1, 1)
        send(f, p, r1, 0, 1, -1)
        send(f, p, r1, 0, None)

    def first_near():
        for f in (0, 1):
            for p, r in ((0, -1), (1, 1)):
                arrived(f, p, r, 0)
                send(f, p, r, 0, 0, -r)
                second_axis(f, p, r)
        for f in (0, 1):
            for p, r in ((1, -1), (0, 1)):
                arrived(f, p, r, 0)
                second_axis(f, p, r)

    def first_far():
        for f in (0, 1):
            for p in (0, 1):
                arrived(f, p, far, 0)
                second_axis(f, p, far)

    def second_near(r1):
        for f in (0, 1):
            for p, r in ((0, -1), (1, 1)):
                arrived(f, p, r1, r)
                send(f, p, r1, r, 1, -r)
                send(f, p, r1, r, None)
        for f in (0, 1):
            for p, r in ((1, -1), (0, 1)):
                arrived(f, p, r1, r)
                send(f, p, r1, r, None)

    def second_far(r1):
        for f in (0, 1):
            for p in (0, 1):
                arrived(f, p, r1, far)
                send(f, p, r1, far, None)

    first_near()
    dw1[...] = jnp.zeros_like(dw1)
    dw3[...] = jnp.zeros_like(dw3)
    dw2[...] = jnp.zeros_like(dw2)
    second_near(0)
    first_far()
    second_far(0)
    second_near(-1)
    second_near(1)
    second_near(far)
    second_far(-1)
    second_far(1)
    second_far(far)

    def plane(b, carry):
        home = b * 2 + 1 - core
        for f in (0, 1):
            for p in (0, 1):
                src = dyall.at[home, f, pl.ds(p * piece, piece)]
                pltpu.make_async_copy(src, src, ag_recv2.at[b, f, p]).wait()
        for p in (0, 1):
            t = tab.at[home, pl.ds(p * top, top)]
            pltpu.make_async_copy(t, t, tb_recv2.at[b, p]).wait()
        return carry

    lax.fori_loop(0, side * side, plane, 0)
    for cp in wloads:
        cp.wait()

    def compute(k, bx, by):
        s = k % 2
        for cp in stream(k):
            cp.wait()

        @pl.when(k + 1 < len(ORDER))
        def _():
            for cp in stream(k + 1):
                cp.start()

        slot_row = lax.broadcasted_iota(jnp.int32, (capacity, tokens), 0).astype(F32)
        base = (me * capacity).astype(F32)
        for i in (0, 1):
            home = block(bx, by) * 2 + i
            rel = tab[home, 0:top, :] - base
            mine = (rel >= 0.0) & (rel < float(capacity))
            slot = jnp.max(jnp.where(mine, rel, -1.0), axis=0, keepdims=True)
            gate = jnp.sum(jnp.where(mine, tab[home, top:2 * top, :], 0.0), axis=0, keepdims=True)
            hit = slot_row == slot
            row_gate = jnp.sum(jnp.where(hit, gate, 0.0), axis=1, keepdims=True)
            hit = jnp.where(hit, 1.0, 0.0).astype(BF16)
            for f in (0, 1):
                picked = mm(hit, dyall[home, f], ((1,), (0,)))
                dyd[i * capacity:(i + 1) * capacity, f * half:(f + 1) * half] = (row_gate * picked).astype(BF16)
        dyv = dyd[...]
        d_act = mm(dyv, w2[...], ((1,), (1,))).astype(BF16).astype(F32)
        g = h1b[s].astype(F32)
        u = h3b[s].astype(F32)
        sg = jax.nn.sigmoid(g)
        silu = g * sg
        act = (silu * u).astype(BF16)
        dh[:, 0:ff] = (d_act * u * sg * (1.0 + g * (1.0 - sg))).astype(BF16)
        dh[:, ff:2 * ff] = (d_act * silu).astype(BF16)
        dh1 = dh[:, 0:ff]
        dh3 = dh[:, ff:2 * ff]
        for f in (0, 1):
            cols = pl.ds(f * half, half)
            d_x = (mm(dh1, w1[cols, :], ((1,), (1,))) + mm(dh3, w3[cols, :], ((1,), (1,)))).astype(BF16)
            for i in (0, 1):
                dxs[f, block(bx, by) * 2 + i] = d_x[i * capacity:(i + 1) * capacity, :]
        dw2[...] += mm(act, dyv, ((0,), (0,)))
        dw1[...] += mm(xb[s], dh1, ((0,), (0,)))
        dw3[...] += mm(xb[s], dh3, ((0,), (0,)))

    def target(f, sign, c):
        return device(wrap(x + sign), y, c) if f == 0 else device(x, wrap(y + sign), c)

    def send_rows(k, bx, by):
        for f in (0, 1):
            d = pick(k, [o[f] for o in ORDER])
            pos = x if f == 0 else y
            other = by if f == 0 else bx
            slot_near = other * row_len + pos * 2 + core
            for cc in (0, 1):
                home = block(bx, by) * 2 + cc
                same = core == cc
                local = (d == 0) & same

                @pl.when(local)
                def _():
                    rcv[f, slot_near] = dxs[f, home]

                @pl.when(jnp.logical_not(local))
                def _():
                    plus = (d == 1) | ((d == far) & same)
                    sign = jnp.where(d == 0, 0, jnp.where(plus, 1, -1))
                    slot = jnp.where(d == far, side * row_len + jnp.where(same, 0, side) + other, slot_near)
                    pltpu.make_async_remote_copy(dxs.at[f, home], rcv.at[f, slot], r_send, r_recv.at[f, slot],
                                                 device_id=target(f, sign, cc)).start()

    def relay_rows(f, other):
        pos = x if f == 0 else y
        for sign in (1, -1):
            slot_in = side * row_len + (0 if sign == 1 else side) + other
            src_core = core if sign == 1 else 1 - core
            slot_out = other * row_len + wrap(pos - sign) * 2 + src_core
            cp = pltpu.make_async_remote_copy(rcv.at[f, slot_in], rcv.at[f, slot_out], rl_send,
                                              r_recv.at[f, slot_in], device_id=target(f, sign, core))
            cp.wait_recv()
            pltpu.make_async_remote_copy(rcv.at[f, slot_in], rcv.at[f, slot_out], rl_send,
                                         r_recv.at[f, slot_out], device_id=target(f, sign, core)).start()

    def sums(f, d):
        pos = x if f == 0 else y
        hx, hy = (x, wrap(y + d)) if f == 0 else (wrap(x + d), y)
        other = hy if f == 0 else hx
        home = block(hx, hy) * 2 + core
        code = tab[home, 0:top, :]
        slot_row = lax.broadcasted_iota(jnp.int32, (capacity, tokens), 0).astype(F32)
        for s in range(row_len):
            @pl.when(pos * 2 + core != s)
            def _():
                ref = rcv.at[f, other * row_len + s]
                pltpu.make_async_copy(ref, ref, r_recv.at[f, other * row_len + s]).wait()

            e = y * row_len + s if f == 0 else ((s // 2) * side + x) * 2 + s % 2
            rel = code - (e * capacity).astype(F32)
            slot = jnp.max(jnp.where((rel >= 0.0) & (rel < float(capacity)), rel, -1.0), axis=0, keepdims=True)
            hitb[s * capacity:(s + 1) * capacity, :] = jnp.where(slot_row == slot, 1.0, 0.0).astype(BF16)
        data = rcv[f, pl.ds(other * row_len, row_len)].reshape(row_len * capacity, half)
        return mm(hitb[...], data, ((0,), (0,)))

    def send_sums(f, d):
        axis = 1 - f
        if d == far:
            for i, sign in ((0, 1), (1, -1)):
                pltpu.make_async_remote_copy(psend.at[f, d - 1, pl.ds(i * piece, piece)], prelay.at[f, i], p_send,
                                             pl_recv.at[f, i], device_id=target(axis, sign, core)).start()
        else:
            sign = 1 if d == 1 else -1
            pltpu.make_async_remote_copy(psend.at[f, d - 1], precv.at[f, d - 1], p_send, p_recv.at[f, d - 1],
                                         device_id=target(axis, sign, core)).start()

    def far_sum(f, i):
        return precv.at[f, far - 1, pl.ds(i * piece, piece)], p_recv.at[f, far - 1 if i == 0 else side - 1]

    def relay_sums(f):
        for i, sign in ((0, 1), (1, -1)):
            src = prelay.at[f, i]
            pltpu.make_async_copy(src, src, pl_recv.at[f, i]).wait()
            dst, sem = far_sum(f, i)
            pltpu.make_async_remote_copy(src, dst, pl_send, sem, device_id=target(1 - f, sign, core)).start()

    def step(k, carry):
        @pl.when(k < len(ORDER))
        def _():
            bx = wrap(x + pick(k, [o[0] for o in ORDER]))
            by = wrap(y + pick(k, [o[1] for o in ORDER]))
            compute(k, bx, by)
            send_rows(k, bx, by)

        late = k - RELAY_LAG
        ox = pick(late, [o[0] for o in ORDER])
        oy = pick(late, [o[1] for o in ORDER])
        live = (late >= 0) & (late < len(ORDER))

        @pl.when(live & (ox == far))
        def _():
            relay_rows(0, wrap(y + oy))

        @pl.when(live & (oy == far))
        def _():
            relay_rows(1, wrap(x + ox))

        for at, f, d in SUMS:
            @pl.when(k == at)
            def _():
                total = sums(f, d)
                if d == 0:
                    pown[f] = total
                else:
                    psend[f, d - 1] = total
                    send_sums(f, d)

        for at, f in SUM_RELAYS:
            @pl.when(k == at)
            def _():
                relay_sums(f)

        return carry

    lax.fori_loop(0, len(ORDER), step, 0)
    outs = [pltpu.make_async_copy(a, b, out_sem.at[i]) for i, (a, b) in enumerate(((dw1, dw1_ref), (dw3, dw3_ref), (dw2, dw2_ref)))]
    for cp in outs:
        cp.start()
    lax.fori_loop(len(ORDER), STEPS, step, 0)

    for f in (0, 1):
        total = pown[f]
        for d in range(1, side):
            if d == far:
                for i in (0, 1):
                    dst, sem = far_sum(f, i)
                    pltpu.make_async_copy(dst, dst, sem).wait()
            else:
                ref = precv.at[f, d - 1]
                pltpu.make_async_copy(ref, ref, p_recv.at[f, d - 1]).wait()
            total = total + precv[f, d - 1]
        dx_ref[:, f * half:(f + 1) * half] = total.astype(BF16)

    def drained(ref, sem):
        pltpu.make_async_copy(ref, ref, sem).wait()

    chips = side * side
    drained(dyall.at[pl.ds(0, 2 * chips - 1)], ag_send)
    drained(tab.at[pl.ds(0, 2 * chips - 1)], tb_send)
    drained(dxs.at[:, pl.ds(0, 2 * chips - side)], r_send)
    drained(dxs.at[:, pl.ds(0, 2 * side)], rl_send)
    drained(psend, p_send)
    drained(prelay, pl_send)
    for cp in outs:
        cp.wait()


def dgates_kernel(dy_ref, yb_ref, out_ref):
    out_ref[...] = jnp.sum(dy_ref[...].astype(F32)[:, None, :] * yb_ref[...].astype(F32), axis=2)


def solution(mesh):
    ep_size = mesh.shape['ep']
    side = math.isqrt(ep_size // 2)
    tok_spec = P(('dp', 'ep'), None)
    buf_spec = P(('dp', 'ep'), None, None)
    expert_spec = P('ep', None, None)

    def device_step(dy, topk_idx, slot_idx, gates, y_back, x_disp, h1_disp, h3_disp, w_gate, w_up, w_down):
        capacity = x_disp.shape[1] // ep_size
        tokens, d = dy.shape
        top = gates.shape[1]
        ff = w_gate.shape[2]
        half = d // 2
        rows = 2 * capacity
        row_len = 2 * side

        code = jnp.where(slot_idx >= 0, topk_idx * capacity + slot_idx, -1).astype(F32)
        tab = jnp.concatenate([code, gates], axis=1).T

        tb = min(32, tokens)
        d_gates = pl.pallas_call(
            dgates_kernel, grid=(tokens // tb,),
            in_specs=[pl.BlockSpec((tb, d), lambda i: (i, 0)), pl.BlockSpec((tb, top, d), lambda i: (i, 0, 0))],
            out_specs=pl.BlockSpec((tb, top), lambda i: (i, 0)),
            out_shape=jax.ShapeDtypeStruct((tokens, top), F32), name='dgates',
        )(dy, y_back)

        vm = pltpu.VMEM
        dma = pltpu.SemaphoreType.DMA
        any_spec = pl.BlockSpec(memory_space=pl.ANY)
        dx, dw1, dw3, dw2 = pl.pallas_call(
            functools.partial(kernel_body, side, capacity),
            in_specs=[any_spec] * 8,
            out_specs=[pl.BlockSpec(memory_space=pltpu.VMEM)] + [any_spec] * 3,
            out_shape=[jax.ShapeDtypeStruct((tokens, d), BF16),
                       jax.ShapeDtypeStruct((d, ff), F32), jax.ShapeDtypeStruct((d, ff), F32),
                       jax.ShapeDtypeStruct((ff, d), F32)],
            scratch_shapes=[
                vm((ep_size, 2, tokens, half), BF16), vm((ep_size, 2 * top, tokens), F32),
                vm((d, ff), BF16), vm((d, ff), BF16), vm((ff, d), BF16),
                vm((d, ff), F32), vm((d, ff), F32), vm((ff, d), F32),
                vm((2, rows, d), BF16), vm((2, rows, ff), BF16), vm((2, rows, ff), BF16),
                vm((rows, d), BF16), vm((rows, 2 * ff), BF16),
                vm((2, ep_size, capacity, half), BF16),
                vm((2, side * row_len + 2 * side, capacity, half), BF16),
                vm((row_len * capacity, tokens), BF16),
                vm((2, side - 1, tokens, half), F32), vm((2, tokens, half), F32),
                vm((2, side - 1, tokens, half), F32), vm((2, 2, tokens // 2, half), F32),
                dma((3,)), dma((3,)), dma((2, 3)), dma((3,)),
                dma, dma((side * side, 2, 2)), dma((side * side, 2, 2)),
                dma, dma((side * side, 2)), dma((side * side, 2)),
                dma, dma((2, side * row_len + 2 * side)), dma,
                dma, dma((2, side)), dma, dma((2, 2)),
            ],
            compiler_params=pltpu.CompilerParams(collective_id=0, has_side_effects=True, vmem_limit_bytes=67043328),
            name='moe_bwd',
        )(dy, tab, x_disp[0], h1_disp[0], h3_disp[0], w_gate[0], w_up[0], w_down[0])
        return dx, d_gates, dw1[None], dw3[None], dw2[None]

    return jax.shard_map(
        device_step, mesh=mesh,
        in_specs=(tok_spec, tok_spec, tok_spec, tok_spec, buf_spec, buf_spec, buf_spec, buf_spec,
                  expert_spec, expert_spec, expert_spec),
        out_specs=(tok_spec, tok_spec, buf_spec, buf_spec, buf_spec),
        check_vma=False)
```

```python
import functools
import math

import jax
import jax.numpy as jnp
from jax import lax
from jax.experimental import pallas as pl
from jax.experimental.pallas import tpu as pltpu
from jax.sharding import PartitionSpec as P

F32 = jnp.float32
BF16 = jnp.bfloat16

ORDER = ((2, 2), (2, 1), (1, 2), (2, 3), (3, 2), (2, 0), (0, 2),
         (1, 1), (1, 3), (3, 1), (1, 0), (0, 1), (3, 3), (3, 0), (0, 3), (0, 0))
SUMS = ((8, 1, 2), (9, 0, 2), (13, 1, 1), (14, 0, 1), (16, 1, 3), (17, 0, 3), (18, 1, 0), (19, 0, 0))
STEPS = 20


def mm(a, b, dims):
    return lax.dot_general(a, b, (dims, ((), ())), preferred_element_type=F32)


def pick(k, values):
    out = jnp.int32(values[0])
    for i, v in enumerate(values[1:], 1):
        out = jnp.where(k == i, jnp.int32(v), out)
    return out


def kernel_body(side, capacity, dy_ref, topk_ref, slot_ref, gates_ref, yb_ref, x_ref, h1_ref, h3_ref, w1_ref, w3_ref, w2_ref,
                dx_ref, dg_ref, dw1_ref, dw3_ref, dw2_ref,
                dyall, tab, w1, w3, w2, dw1, dw3, dw2, xb, h1b, h3b, dyd, dh, dxs, rcv, hitb, topk, slots, yb, dg,
                psend, pown, precv, prelay,
                load_sem, w_sem, yb_sem, in_sem, out_sem, ag_send, ag_recv, ag_recv2, tb_send, tb_recv, tb_recv2,
                r_send, r_recv, p_send, p_recv, pl_recv):
    tokens = dyall.shape[2]
    top = tab.shape[1] // 2
    half = dyall.shape[3]
    ff = h1b.shape[2]
    rows = 2 * capacity
    piece = tokens // 2
    row_len = 2 * side
    me = lax.axis_index('ep')
    core = me % 2
    x = (me // 2) % side
    y = me // (2 * side)
    far = side // 2

    def wrap(v):
        return (v + side) % side

    def block(bx, by):
        return by * side + bx

    def device(bx, by, c):
        return {'ep': block(bx, by) * 2 + c}

    def chip(f, r1, r2):
        return (wrap(x + r1), wrap(y + r2)) if f == 0 else (wrap(x + r2), wrap(y + r1))

    loads = [pltpu.make_async_copy(dy_ref.at[:, pl.ds(f * half, half)], dyall.at[me, f], load_sem.at[f]) for f in (0, 1)]
    loads += [pltpu.make_async_copy(a, b, load_sem.at[2 + i]) for i, (a, b) in enumerate((
        (topk_ref, topk), (slot_ref, slots), (gates_ref, tab.at[me, pl.ds(top, top)])))]
    wloads = [pltpu.make_async_copy(a, b, w_sem.at[i]) for i, (a, b) in enumerate(((w1_ref, w1), (w3_ref, w3), (w2_ref, w2)))]
    for cp in loads + wloads:
        cp.start()

    chunk = yb.shape[1]
    yb_loads = [pltpu.make_async_copy(yb_ref.at[pl.ds(i * chunk, chunk)], yb.at[i % 2], yb_sem.at[i % 2])
                for i in range(tokens // chunk)]
    for cp in yb_loads[:2]:
        cp.start()

    def stream(k):
        b = block(wrap(x + pick(k, [o[0] for o in ORDER])), wrap(y + pick(k, [o[1] for o in ORDER])))
        s = k % 2
        src = pl.ds(b * rows, rows)
        return [pltpu.make_async_copy(x_ref.at[src], xb.at[s], in_sem.at[s, 0]),
                pltpu.make_async_copy(h1_ref.at[src], h1b.at[s], in_sem.at[s, 1]),
                pltpu.make_async_copy(h3_ref.at[src], h3b.at[s], in_sem.at[s, 2])]

    for cp in stream(jnp.int32(0)):
        cp.start()

    barrier = pltpu.get_barrier_semaphore()
    peers = [(wrap(x + r), y) for r in range(1, side)] + [(x, wrap(y + r)) for r in range(1, side)]
    for c in (0, 1):
        for bx, by in peers:
            pl.semaphore_signal(barrier, inc=1, device_id=device(bx, by, c))
    pl.semaphore_signal(barrier, inc=1, device_id=device(x, y, 1 - core))
    for cp in loads:
        cp.wait()
    tab[me, 0:top, :] = jnp.where(slots[...] >= 0, topk[...] * capacity + slots[...], -1).astype(F32)
    pl.semaphore_wait(barrier, 2 * len(peers) + 1)

    def gather_copy(f, p, r1, r2, axis, sign):
        bx, by = chip(f, r1, r2)
        home = block(bx, by) * 2 + core
        src = dyall.at[home, f, pl.ds(p * piece, piece)]
        if axis is None:
            dev, rs, ts = device(x, y, 1 - core), ag_recv2, tb_recv2
        else:
            nx, ny = chip(f, sign, 0) if axis == 0 else chip(f, 0, sign)
            dev, rs, ts = device(nx, ny, core), ag_recv, tb_recv
        out = [pltpu.make_async_remote_copy(src, src, ag_send, rs.at[block(bx, by), f, p], device_id=dev)]
        if f == 0:
            t = tab.at[home, pl.ds(p * top, top)]
            out.append(pltpu.make_async_remote_copy(t, t, tb_send, ts.at[block(bx, by), p], device_id=dev))
        return out

    def send(f, p, r1, r2, axis, sign=0):
        for cp in gather_copy(f, p, r1, r2, axis, sign):
            cp.start()

    def arrived(f, p, r1, r2):
        for cp in gather_copy(f, p, r1, r2, 0, 1):
            cp.wait_recv()

    for axis in (0, 1):
        for f in (0, 1):
            for p, sign in ((0, 1), (1, -1), (1, 1), (0, -1)):
                send(f, p, 0, 0, axis, sign)
    for f in (0, 1):
        for p in (0, 1):
            send(f, p, 0, 0, None)

    def second_axis(f, p, r1):
        send(f, p, r1, 0, 1, 1)
        send(f, p, r1, 0, 1, -1)
        send(f, p, r1, 0, None)

    def first_near():
        for f in (0, 1):
            for p, r in ((0, -1), (1, 1)):
                arrived(f, p, r, 0)
                send(f, p, r, 0, 0, -r)
                second_axis(f, p, r)
        for f in (0, 1):
            for p, r in ((1, -1), (0, 1)):
                arrived(f, p, r, 0)
                second_axis(f, p, r)

    def first_far():
        for f in (0, 1):
            for p in (0, 1):
                arrived(f, p, far, 0)
                second_axis(f, p, far)

    def second_near(r1):
        for f in (0, 1):
            for p, r in ((0, -1), (1, 1)):
                arrived(f, p, r1, r)
                send(f, p, r1, r, 1, -r)
                send(f, p, r1, r, None)
        for f in (0, 1):
            for p, r in ((1, -1), (0, 1)):
                arrived(f, p, r1, r)
                send(f, p, r1, r, None)

    def second_far(r1):
        for f in (0, 1):
            for p in (0, 1):
                arrived(f, p, r1, far)
                send(f, p, r1, far, None)

    def gate_grads(i):
        yb_loads[i].wait()
        part = sum(jnp.sum(dyall[me, f, i * chunk:(i + 1) * chunk, :].astype(F32)[:, None, :]
                           * yb[i % 2, :, :, f * half:(f + 1) * half].astype(F32), axis=2) for f in (0, 1))
        dg[i * chunk:(i + 1) * chunk, 0:top] = part
        if i + 2 < len(yb_loads):
            yb_loads[i + 2].start()

    first_near()
    dw1[...] = jnp.zeros_like(dw1)
    dw3[...] = jnp.zeros_like(dw3)
    dw2[...] = jnp.zeros_like(dw2)
    dg[...] = jnp.zeros_like(dg)
    groups = [(second_near, 0), (first_far,), (second_far, 0), (second_near, -1), (second_near, 1),
              (second_near, far), (second_far, -1), (second_far, 1), (second_far, far)]
    for i, group in enumerate(groups):
        group[0](*group[1:])
        if i < len(yb_loads):
            gate_grads(i)
    dg_ref[...] = dg[...].T[0:top, :]

    def plane(b, carry):
        home = b * 2 + 1 - core
        for f in (0, 1):
            for p in (0, 1):
                src = dyall.at[home, f, pl.ds(p * piece, piece)]
                pltpu.make_async_copy(src, src, ag_recv2.at[b, f, p]).wait()
        for p in (0, 1):
            t = tab.at[home, pl.ds(p * top, top)]
            pltpu.make_async_copy(t, t, tb_recv2.at[b, p]).wait()
        return carry

    lax.fori_loop(0, side * side, plane, 0)
    for cp in wloads:
        cp.wait()

    def compute(k, bx, by):
        s = k % 2
        for cp in stream(k):
            cp.wait()

        @pl.when(k + 1 < len(ORDER))
        def _():
            for cp in stream(k + 1):
                cp.start()

        slot_row = lax.broadcasted_iota(jnp.int32, (capacity, tokens), 0).astype(F32)
        base = (me * capacity).astype(F32)
        for i in (0, 1):
            home = block(bx, by) * 2 + i
            rel = tab[home, 0:top, :] - base
            mine = (rel >= 0.0) & (rel < float(capacity))
            slot = jnp.max(jnp.where(mine, rel, -1.0), axis=0, keepdims=True)
            gate = jnp.sum(jnp.where(mine, tab[home, top:2 * top, :], 0.0), axis=0, keepdims=True)
            hit = slot_row == slot
            row_gate = jnp.sum(jnp.where(hit, gate, 0.0), axis=1, keepdims=True)
            hit = jnp.where(hit, 1.0, 0.0).astype(BF16)
            for f in (0, 1):
                picked = mm(hit, dyall[home, f], ((1,), (0,)))
                dyd[i * capacity:(i + 1) * capacity, f * half:(f + 1) * half] = (row_gate * picked).astype(BF16)
        dyv = dyd[...]
        d_act = mm(dyv, w2[...], ((1,), (1,))).astype(BF16).astype(F32)
        g = h1b[s].astype(F32)
        u = h3b[s].astype(F32)
        sg = jax.nn.sigmoid(g)
        silu = g * sg
        act = (silu * u).astype(BF16)
        dh[:, 0:ff] = (d_act * u * sg * (1.0 + g * (1.0 - sg))).astype(BF16)
        dh[:, ff:2 * ff] = (d_act * silu).astype(BF16)
        dh1 = dh[:, 0:ff]
        dh3 = dh[:, ff:2 * ff]
        for f in (0, 1):
            cols = pl.ds(f * half, half)
            d_x = (mm(dh1, w1[cols, :], ((1,), (1,))) + mm(dh3, w3[cols, :], ((1,), (1,)))).astype(BF16)
            for i in (0, 1):
                dxs[f, block(bx, by) * 2 + i] = d_x[i * capacity:(i + 1) * capacity, :]
        dw2[...] += mm(act, dyv, ((0,), (0,)))
        dw1[...] += mm(xb[s], dh1, ((0,), (0,)))
        dw3[...] += mm(xb[s], dh3, ((0,), (0,)))

    def target(f, sign, c):
        return device(wrap(x + sign), y, c) if f == 0 else device(x, wrap(y + sign), c)

    def send_rows(k, bx, by):
        for f in (0, 1):
            d = pick(k, [o[f] for o in ORDER])
            pos = x if f == 0 else y
            other = by if f == 0 else bx
            slot = other * row_len + pos * 2 + core
            for cc in (0, 1):
                home = block(bx, by) * 2 + cc
                local = (d == 0) & (core == cc)

                @pl.when(local)
                def _():
                    rcv[f, slot] = dxs[f, home]

                @pl.when(jnp.logical_not(local))
                def _():
                    pltpu.make_async_remote_copy(dxs.at[f, home], rcv.at[f, slot], r_send, r_recv.at[f, slot],
                                                 device_id=target(f, d, cc)).start()

    def sums(f, d):
        pos = x if f == 0 else y
        hx, hy = (x, wrap(y + d)) if f == 0 else (wrap(x + d), y)
        other = hy if f == 0 else hx
        home = block(hx, hy) * 2 + core
        code = tab[home, 0:top, :]
        slot_row = lax.broadcasted_iota(jnp.int32, (capacity, tokens), 0).astype(F32)
        for s in range(row_len):
            @pl.when(pos * 2 + core != s)
            def _():
                ref = rcv.at[f, other * row_len + s]
                pltpu.make_async_copy(ref, ref, r_recv.at[f, other * row_len + s]).wait()

            e = y * row_len + s if f == 0 else ((s // 2) * side + x) * 2 + s % 2
            rel = code - (e * capacity).astype(F32)
            slot = jnp.max(jnp.where((rel >= 0.0) & (rel < float(capacity)), rel, -1.0), axis=0, keepdims=True)
            hitb[s * capacity:(s + 1) * capacity, :] = jnp.where(slot_row == slot, 1.0, 0.0).astype(BF16)
        data = rcv[f, pl.ds(other * row_len, row_len)].reshape(row_len * capacity, half)
        return mm(hitb[...], data, ((0,), (0,)))

    def send_sums(f, d, total):
        axis = 1 - f
        if d == far:
            psend[f, d - 1] = total
            for i, sign in ((0, 1), (1, -1)):
                pltpu.make_async_remote_copy(psend.at[f, d - 1, pl.ds(i * piece, piece)], prelay.at[f, i], p_send,
                                             pl_recv.at[f, i], device_id=target(axis, sign, core)).start()
        else:
            i, sign = (0, 1) if d == 1 else (1, -1)
            src = prelay.at[f, i]
            pltpu.make_async_copy(src, src, pl_recv.at[f, i]).wait()
            psend[f, d - 1] = total
            psend[f, d - 1, i * piece:(i + 1) * piece, :] = total[i * piece:(i + 1) * piece, :] + prelay[f, i]
            pltpu.make_async_remote_copy(psend.at[f, d - 1], precv.at[f, i], p_send, p_recv.at[f, i],
                                         device_id=target(axis, sign, core)).start()

    def step(k, carry):
        @pl.when(k < len(ORDER))
        def _():
            bx = wrap(x + pick(k, [o[0] for o in ORDER]))
            by = wrap(y + pick(k, [o[1] for o in ORDER]))
            compute(k, bx, by)
            send_rows(k, bx, by)

        for at, f, d in SUMS:
            @pl.when(k == at)
            def _():
                total = sums(f, d)
                if d == 0:
                    pown[f] = total
                else:
                    send_sums(f, d, total)

        return carry

    lax.fori_loop(0, len(ORDER), step, 0)
    outs = [pltpu.make_async_copy(a, b, out_sem.at[i]) for i, (a, b) in enumerate(((dw1, dw1_ref), (dw3, dw3_ref), (dw2, dw2_ref)))]
    for cp in outs:
        cp.start()
    lax.fori_loop(len(ORDER), STEPS, step, 0)

    for f in (0, 1):
        total = pown[f]
        for i in (0, 1):
            ref = precv.at[f, i]
            pltpu.make_async_copy(ref, ref, p_recv.at[f, i]).wait()
            total = total + precv[f, i]
        dx_ref[:, f * half:(f + 1) * half] = total.astype(BF16)

    def drained(ref, sem):
        pltpu.make_async_copy(ref, ref, sem).wait()

    chips = side * side
    drained(dyall.at[pl.ds(0, 2 * chips - 1)], ag_send)
    drained(tab.at[pl.ds(0, 2 * chips - 1)], tb_send)
    drained(dxs.at[:, pl.ds(0, 2 * chips - side)], r_send)
    drained(psend, p_send)
    for cp in outs:
        cp.wait()


def solution(mesh):
    ep_size = mesh.shape['ep']
    side = math.isqrt(ep_size // 2)
    tok_spec = P(('dp', 'ep'), None)
    buf_spec = P(('dp', 'ep'), None, None)
    expert_spec = P('ep', None, None)

    def device_step(dy, topk_idx, slot_idx, gates, y_back, x_disp, h1_disp, h3_disp, w_gate, w_up, w_down):
        capacity = x_disp.shape[1] // ep_size
        tokens, d = dy.shape
        top = gates.shape[1]
        ff = w_gate.shape[2]
        half = d // 2
        rows = 2 * capacity
        row_len = 2 * side

        chunk = tokens // 8
        vm = pltpu.VMEM
        dma = pltpu.SemaphoreType.DMA
        any_spec = pl.BlockSpec(memory_space=pl.ANY)
        dx, d_gates, dw1, dw3, dw2 = pl.pallas_call(
            functools.partial(kernel_body, side, capacity),
            in_specs=[any_spec] * 11,
            out_specs=[pl.BlockSpec(memory_space=pltpu.VMEM)] * 2 + [any_spec] * 3,
            out_shape=[jax.ShapeDtypeStruct((tokens, d), BF16), jax.ShapeDtypeStruct((top, tokens), F32),
                       jax.ShapeDtypeStruct((d, ff), F32), jax.ShapeDtypeStruct((d, ff), F32),
                       jax.ShapeDtypeStruct((ff, d), F32)],
            scratch_shapes=[
                vm((ep_size, 2, tokens, half), BF16), vm((ep_size, 2 * top, tokens), F32),
                vm((d, ff), BF16), vm((d, ff), BF16), vm((ff, d), BF16),
                vm((d, ff), F32), vm((d, ff), F32), vm((ff, d), F32),
                vm((2, rows, d), BF16), vm((2, rows, ff), BF16), vm((2, rows, ff), BF16),
                vm((rows, d), BF16), vm((rows, 2 * ff), BF16),
                vm((2, ep_size, capacity, half), BF16),
                vm((2, side * row_len, capacity, half), BF16),
                vm((row_len * capacity, tokens), BF16),
                vm((top, tokens), jnp.int32), vm((top, tokens), jnp.int32),
                vm((2, chunk, top, d), BF16), vm((tokens, 128), F32),
                vm((2, side - 1, tokens, half), F32), vm((2, tokens, half), F32),
                vm((2, 2, tokens, half), F32), vm((2, 2, tokens // 2, half), F32),
                dma((5,)), dma((3,)), dma((2,)), dma((2, 3)), dma((3,)),
                dma, dma((side * side, 2, 2)), dma((side * side, 2, 2)),
                dma, dma((side * side, 2)), dma((side * side, 2)),
                dma, dma((2, side * row_len)),
                dma, dma((2, 2)), dma((2, 2)),
            ],
            compiler_params=pltpu.CompilerParams(collective_id=0, has_side_effects=True, vmem_limit_bytes=67043328),
            name='moe_bwd',
        )(dy, topk_idx.T, slot_idx.T, gates.T, y_back, x_disp[0], h1_disp[0], h3_disp[0], w_gate[0], w_up[0], w_down[0])
        return dx, d_gates.T, dw1[None], dw3[None], dw2[None]

    return jax.shard_map(
        device_step, mesh=mesh,
        in_specs=(tok_spec, tok_spec, tok_spec, tok_spec, buf_spec, buf_spec, buf_spec, buf_spec,
                  expert_spec, expert_spec, expert_spec),
        out_specs=(tok_spec, tok_spec, buf_spec, buf_spec, buf_spec),
        check_vma=False)
```

```python
import functools
import math

import jax
import jax.numpy as jnp
from jax import lax
from jax.experimental import pallas as pl
from jax.experimental.pallas import tpu as pltpu
from jax.sharding import PartitionSpec as P

F32 = jnp.float32
BF16 = jnp.bfloat16

ORDER = ((0, 0), (1, 0), (3, 0), (0, 1), (0, 3), (2, 0), (0, 2),
         (1, 1), (3, 3), (1, 3), (3, 1), (2, 2), (2, 1), (1, 2), (2, 3), (3, 2))
SENDS = ((0, 1, 2, 3, 4, 5, 6, 7, 8, -1, -1, 11, 12, 13, 14, 15, -1, -1, -1, -1, -1, -1, -1, -1),
         (-1, -1, -1, -1, -1, -1, -1, -1, -1, -1, -1, -1, -1, -1, 9, 10, -1, -1, -1, -1, -1, -1, -1, -1))
SUMS = ((9, 0, 0), (10, 1, 0), (16, 1, 2), (17, 0, 2), (18, 1, 1), (19, 0, 1), (20, 1, 3), (21, 0, 3))
JOINS = ((22, 1), (23, 0))
GROUPS = ((1, 'first_near'), (1, 'gates'), (1, 'second_near', 0), (3, 'first_far'), (4, 'second_near', -1),
          (5, 'second_far', 0), (5, 'second_near', 1), (7, 'second_near', 2), (9, 'second_far', -1),
          (10, 'second_far', 1), (11, 'second_far', 2))
STEPS = 24


def mm(a, b, dims):
    return lax.dot_general(a, b, (dims, ((), ())), preferred_element_type=F32)


def pick(k, values):
    out = jnp.int32(values[0])
    for i, v in enumerate(values[1:], 1):
        out = jnp.where(k == i, jnp.int32(v), out)
    return out


def kernel_body(side, capacity, dy_ref, topk_ref, slot_ref, gates_ref, yb_ref, x_ref, h1_ref, h3_ref, w1_ref, w3_ref, w2_ref,
                dx_ref, dg_ref, dw1_ref, dw3_ref, dw2_ref,
                dyall, tab, w1, w3, w2, dw1, dw3, dw2, xb, h1b, h3b, dyd, dh, dxs, rcv, hitb, topk, slots, yb, dg,
                psend, pown, precv, prelay,
                load_sem, w_sem, yb_sem, in_sem, out_sem, ag_send, ag_recv, ag_recv2, tb_send, tb_recv, tb_recv2,
                r_send, r_recv, p_send, p_recv, pl_recv):
    tokens = dyall.shape[2]
    top = tab.shape[1] // 2
    half = dyall.shape[3]
    ff = h1b.shape[2]
    rows = 2 * capacity
    piece = tokens // 2
    row_len = 2 * side
    me = lax.axis_index('ep')
    core = me % 2
    x = (me // 2) % side
    y = me // (2 * side)
    far = side // 2

    def wrap(v):
        return (v + side) % side

    def block(bx, by):
        return by * side + bx

    def device(bx, by, c):
        return {'ep': block(bx, by) * 2 + c}

    def chip(f, r1, r2):
        return (wrap(x + r1), wrap(y + r2)) if f == 0 else (wrap(x + r2), wrap(y + r1))

    loads = [pltpu.make_async_copy(dy_ref.at[:, pl.ds(f * half, half)], dyall.at[me, f], load_sem.at[f]) for f in (0, 1)]
    loads += [pltpu.make_async_copy(a, b, load_sem.at[2 + i]) for i, (a, b) in enumerate((
        (topk_ref, topk), (slot_ref, slots), (gates_ref, tab.at[me, pl.ds(top, top)])))]
    wloads = [pltpu.make_async_copy(a, b, w_sem.at[i]) for i, (a, b) in enumerate(((w1_ref, w1), (w3_ref, w3), (w2_ref, w2)))]
    for cp in loads + wloads:
        cp.start()

    chunk = yb.shape[1]
    yb_loads = [pltpu.make_async_copy(yb_ref.at[pl.ds(i * chunk, chunk)], yb.at[i % 2], yb_sem.at[i % 2])
                for i in range(tokens // chunk)]
    for cp in yb_loads[:2]:
        cp.start()

    def stream(k):
        b = block(wrap(x + pick(k, [o[0] for o in ORDER])), wrap(y + pick(k, [o[1] for o in ORDER])))
        s = k % 2
        src = pl.ds(b * rows, rows)
        return [pltpu.make_async_copy(x_ref.at[src], xb.at[s], in_sem.at[s, 0]),
                pltpu.make_async_copy(h1_ref.at[src], h1b.at[s], in_sem.at[s, 1]),
                pltpu.make_async_copy(h3_ref.at[src], h3b.at[s], in_sem.at[s, 2])]

    for cp in stream(jnp.int32(0)):
        cp.start()

    barrier = pltpu.get_barrier_semaphore()
    peers = [(wrap(x + r), y) for r in range(1, side)] + [(x, wrap(y + r)) for r in range(1, side)]
    for c in (0, 1):
        for bx, by in peers:
            pl.semaphore_signal(barrier, inc=1, device_id=device(bx, by, c))
    pl.semaphore_signal(barrier, inc=1, device_id=device(x, y, 1 - core))
    for cp in loads:
        cp.wait()
    tab[me, 0:top, :] = jnp.where(slots[...] >= 0, topk[...] * capacity + slots[...], -1).astype(F32)
    pl.semaphore_wait(barrier, 2 * len(peers) + 1)

    def gather_copy(f, p, r1, r2, axis, sign):
        bx, by = chip(f, r1, r2)
        home = block(bx, by) * 2 + core
        src = dyall.at[home, f, pl.ds(p * piece, piece)]
        if axis is None:
            dev, rs, ts = device(x, y, 1 - core), ag_recv2, tb_recv2
        else:
            nx, ny = chip(f, sign, 0) if axis == 0 else chip(f, 0, sign)
            dev, rs, ts = device(nx, ny, core), ag_recv, tb_recv
        out = [pltpu.make_async_remote_copy(src, src, ag_send, rs.at[block(bx, by), f, p], device_id=dev)]
        if f == 0:
            t = tab.at[home, pl.ds(p * top, top)]
            out.append(pltpu.make_async_remote_copy(t, t, tb_send, ts.at[block(bx, by), p], device_id=dev))
        return out

    def send(f, p, r1, r2, axis, sign=0):
        for cp in gather_copy(f, p, r1, r2, axis, sign):
            cp.start()

    def arrived(f, p, r1, r2):
        for cp in gather_copy(f, p, r1, r2, 0, 1):
            cp.wait_recv()

    for axis in (0, 1):
        for f in (0, 1):
            for p, sign in ((0, 1), (1, -1), (1, 1), (0, -1)):
                send(f, p, 0, 0, axis, sign)
    for f in (0, 1):
        for p in (0, 1):
            send(f, p, 0, 0, None)

    def second_axis(f, p, r1):
        send(f, p, r1, 0, 1, 1)
        send(f, p, r1, 0, 1, -1)
        send(f, p, r1, 0, None)

    def first_near():
        for f in (0, 1):
            for p, r in ((0, -1), (1, 1)):
                arrived(f, p, r, 0)
                send(f, p, r, 0, 0, -r)
                second_axis(f, p, r)
        for f in (0, 1):
            for p, r in ((1, -1), (0, 1)):
                arrived(f, p, r, 0)
                second_axis(f, p, r)

    def first_far():
        for f in (0, 1):
            for p in (0, 1):
                arrived(f, p, far, 0)
                second_axis(f, p, far)

    def second_near(r1):
        for f in (0, 1):
            for p, r in ((0, -1), (1, 1)):
                arrived(f, p, r1, r)
                send(f, p, r1, r, 1, -r)
                send(f, p, r1, r, None)
        for f in (0, 1):
            for p, r in ((1, -1), (0, 1)):
                arrived(f, p, r1, r)
                send(f, p, r1, r, None)

    def second_far(r1):
        for f in (0, 1):
            for p in (0, 1):
                arrived(f, p, r1, far)
                send(f, p, r1, far, None)

    def gate_grads(i):
        yb_loads[i].wait()
        part = sum(jnp.sum(dyall[me, f, i * chunk:(i + 1) * chunk, :].astype(F32)[:, None, :]
                           * yb[i % 2, :, :, f * half:(f + 1) * half].astype(F32), axis=2) for f in (0, 1))
        dg[i * chunk:(i + 1) * chunk, 0:top] = part
        if i + 2 < len(yb_loads):
            yb_loads[i + 2].start()

    def gate_grads():
        for i, load in enumerate(yb_loads):
            load.wait()
            part = sum(jnp.sum(dyall[me, f, i * chunk:(i + 1) * chunk, :].astype(F32)[:, None, :]
                               * yb[i % 2, :, :, f * half:(f + 1) * half].astype(F32), axis=2) for f in (0, 1))
            dg[i * chunk:(i + 1) * chunk, 0:top] = part
            if i + 2 < len(yb_loads):
                yb_loads[i + 2].start()
        dg_ref[...] = dg[...].T[0:top, :]

    run = {'first_near': first_near, 'first_far': first_far, 'second_near': second_near,
           'second_far': second_far, 'gates': gate_grads}

    dw1[...] = jnp.zeros_like(dw1)
    dw3[...] = jnp.zeros_like(dw3)
    dw2[...] = jnp.zeros_like(dw2)
    dg[...] = jnp.zeros_like(dg)

    def plane(b):
        home = b * 2 + 1 - core
        for f in (0, 1):
            for p in (0, 1):
                src = dyall.at[home, f, pl.ds(p * piece, piece)]
                pltpu.make_async_copy(src, src, ag_recv2.at[b, f, p]).wait()
        for p in (0, 1):
            t = tab.at[home, pl.ds(p * top, top)]
            pltpu.make_async_copy(t, t, tb_recv2.at[b, p]).wait()

    for cp in wloads:
        cp.wait()

    def compute(k, bx, by):
        s = k % 2
        plane(block(bx, by))
        for cp in stream(k):
            cp.wait()

        @pl.when(k + 1 < len(ORDER))
        def _():
            for cp in stream(k + 1):
                cp.start()

        slot_row = lax.broadcasted_iota(jnp.int32, (capacity, tokens), 0).astype(F32)
        base = (me * capacity).astype(F32)
        for i in (0, 1):
            home = block(bx, by) * 2 + i
            rel = tab[home, 0:top, :] - base
            mine = (rel >= 0.0) & (rel < float(capacity))
            slot = jnp.max(jnp.where(mine, rel, -1.0), axis=0, keepdims=True)
            gate = jnp.sum(jnp.where(mine, tab[home, top:2 * top, :], 0.0), axis=0, keepdims=True)
            hit = slot_row == slot
            row_gate = jnp.sum(jnp.where(hit, gate, 0.0), axis=1, keepdims=True)
            hit = jnp.where(hit, 1.0, 0.0).astype(BF16)
            for f in (0, 1):
                picked = mm(hit, dyall[home, f], ((1,), (0,)))
                dyd[i * capacity:(i + 1) * capacity, f * half:(f + 1) * half] = (row_gate * picked).astype(BF16)
        dyv = dyd[...]
        d_act = mm(dyv, w2[...], ((1,), (1,))).astype(BF16).astype(F32)
        g = h1b[s].astype(F32)
        u = h3b[s].astype(F32)
        sg = jax.nn.sigmoid(g)
        silu = g * sg
        act = (silu * u).astype(BF16)
        dh[:, 0:ff] = (d_act * u * sg * (1.0 + g * (1.0 - sg))).astype(BF16)
        dh[:, ff:2 * ff] = (d_act * silu).astype(BF16)
        dh1 = dh[:, 0:ff]
        dh3 = dh[:, ff:2 * ff]
        for f in (0, 1):
            cols = pl.ds(f * half, half)
            d_x = (mm(dh1, w1[cols, :], ((1,), (1,))) + mm(dh3, w3[cols, :], ((1,), (1,)))).astype(BF16)
            for i in (0, 1):
                dxs[f, block(bx, by) * 2 + i] = d_x[i * capacity:(i + 1) * capacity, :]
        dw2[...] += mm(act, dyv, ((0,), (0,)))
        dw1[...] += mm(xb[s], dh1, ((0,), (0,)))
        dw3[...] += mm(xb[s], dh3, ((0,), (0,)))

    def target(f, sign, c):
        return device(wrap(x + sign), y, c) if f == 0 else device(x, wrap(y + sign), c)

    def send_rows(k):
        bx = wrap(x + pick(k, [o[0] for o in ORDER]))
        by = wrap(y + pick(k, [o[1] for o in ORDER]))
        for f in (0, 1):
            d = pick(k, [o[f] for o in ORDER])
            pos = x if f == 0 else y
            other = by if f == 0 else bx
            slot = other * row_len + pos * 2 + core
            for cc in (0, 1):
                home = block(bx, by) * 2 + cc
                local = (d == 0) & (core == cc)

                @pl.when(local)
                def _():
                    rcv[f, slot] = dxs[f, home]

                @pl.when(jnp.logical_not(local))
                def _():
                    pltpu.make_async_remote_copy(dxs.at[f, home], rcv.at[f, slot], r_send, r_recv.at[f, slot],
                                                 device_id=target(f, d, cc)).start()

    def sums(f, d):
        pos = x if f == 0 else y
        hx, hy = (x, wrap(y + d)) if f == 0 else (wrap(x + d), y)
        other = hy if f == 0 else hx
        home = block(hx, hy) * 2 + core
        code = tab[home, 0:top, :]
        slot_row = lax.broadcasted_iota(jnp.int32, (capacity, tokens), 0).astype(F32)
        for s in range(row_len):
            @pl.when(pos * 2 + core != s)
            def _():
                ref = rcv.at[f, other * row_len + s]
                pltpu.make_async_copy(ref, ref, r_recv.at[f, other * row_len + s]).wait()

            e = y * row_len + s if f == 0 else ((s // 2) * side + x) * 2 + s % 2
            rel = code - (e * capacity).astype(F32)
            slot = jnp.max(jnp.where((rel >= 0.0) & (rel < float(capacity)), rel, -1.0), axis=0, keepdims=True)
            hitb[s * capacity:(s + 1) * capacity, :] = jnp.where(slot_row == slot, 1.0, 0.0).astype(BF16)
        data = rcv[f, pl.ds(other * row_len, row_len)].reshape(row_len * capacity, half)
        return mm(hitb[...], data, ((0,), (0,)))

    def send_sums(f, d, total):
        axis = 1 - f
        if d == far:
            psend[f, d - 1] = total
            for i, sign in ((0, 1), (1, -1)):
                pltpu.make_async_remote_copy(psend.at[f, d - 1, pl.ds(i * piece, piece)], prelay.at[f, i], p_send,
                                             pl_recv.at[f, i], device_id=target(axis, sign, core)).start()
        else:
            i, sign = (0, 1) if d == 1 else (1, -1)
            psend[f, d - 1] = total
            part = pl.ds((1 - i) * piece, piece)
            pltpu.make_async_remote_copy(psend.at[f, d - 1, part], precv.at[f, i, part], p_send, p_recv.at[f, i, 1 - i],
                                         device_id=target(axis, sign, core)).start()

    def join_sums(f):
        for i, sign, d in ((0, 1, 1), (1, -1, side - 1)):
            src = prelay.at[f, i]
            pltpu.make_async_copy(src, src, pl_recv.at[f, i]).wait()
            part = pl.ds(i * piece, piece)
            psend[f, d - 1, part] = psend[f, d - 1, part] + prelay[f, i]
            pltpu.make_async_remote_copy(psend.at[f, d - 1, part], precv.at[f, i, part], p_send, p_recv.at[f, i, i],
                                         device_id=target(1 - f, sign, core)).start()

    def step(k, carry):
        for at, name, *arg in GROUPS:
            @pl.when(k == at)
            def _():
                run[name](*arg)

        @pl.when(k < len(ORDER))
        def _():
            bx = wrap(x + pick(k, [o[0] for o in ORDER]))
            by = wrap(y + pick(k, [o[1] for o in ORDER]))
            compute(k, bx, by)

        for sends in SENDS:
            which = pick(k, sends)

            @pl.when(which >= 0)
            def _():
                send_rows(which)

        for at, f, d in SUMS:
            @pl.when(k == at)
            def _():
                total = sums(f, d)
                if d == 0:
                    pown[f] = total
                else:
                    send_sums(f, d, total)

        for at, f in JOINS:
            @pl.when(k == at)
            def _():
                join_sums(f)

        return carry

    lax.fori_loop(0, len(ORDER), step, 0)
    outs = [pltpu.make_async_copy(a, b, out_sem.at[i]) for i, (a, b) in enumerate(((dw1, dw1_ref), (dw3, dw3_ref), (dw2, dw2_ref)))]
    for cp in outs:
        cp.start()
    lax.fori_loop(len(ORDER), STEPS, step, 0)

    for f in (0, 1):
        total = pown[f]
        for i in (0, 1):
            for p in (0, 1):
                ref = precv.at[f, i, pl.ds(p * piece, piece)]
                pltpu.make_async_copy(ref, ref, p_recv.at[f, i, p]).wait()
            total = total + precv[f, i]
        dx_ref[:, f * half:(f + 1) * half] = total.astype(BF16)

    def drained(ref, sem):
        pltpu.make_async_copy(ref, ref, sem).wait()

    chips = side * side
    drained(dyall.at[pl.ds(0, 2 * chips - 1)], ag_send)
    drained(tab.at[pl.ds(0, 2 * chips - 1)], tb_send)
    drained(dxs.at[:, pl.ds(0, 2 * chips - side)], r_send)
    drained(psend, p_send)
    for cp in outs:
        cp.wait()


def solution(mesh):
    ep_size = mesh.shape['ep']
    side = math.isqrt(ep_size // 2)
    tok_spec = P(('dp', 'ep'), None)
    buf_spec = P(('dp', 'ep'), None, None)
    expert_spec = P('ep', None, None)

    def device_step(dy, topk_idx, slot_idx, gates, y_back, x_disp, h1_disp, h3_disp, w_gate, w_up, w_down):
        capacity = x_disp.shape[1] // ep_size
        tokens, d = dy.shape
        top = gates.shape[1]
        ff = w_gate.shape[2]
        half = d // 2
        rows = 2 * capacity
        row_len = 2 * side

        chunk = tokens // 8
        vm = pltpu.VMEM
        dma = pltpu.SemaphoreType.DMA
        any_spec = pl.BlockSpec(memory_space=pl.ANY)
        dx, d_gates, dw1, dw3, dw2 = pl.pallas_call(
            functools.partial(kernel_body, side, capacity),
            in_specs=[any_spec] * 11,
            out_specs=[pl.BlockSpec(memory_space=pltpu.VMEM)] * 2 + [any_spec] * 3,
            out_shape=[jax.ShapeDtypeStruct((tokens, d), BF16), jax.ShapeDtypeStruct((top, tokens), F32),
                       jax.ShapeDtypeStruct((d, ff), F32), jax.ShapeDtypeStruct((d, ff), F32),
                       jax.ShapeDtypeStruct((ff, d), F32)],
            scratch_shapes=[
                vm((ep_size, 2, tokens, half), BF16), vm((ep_size, 2 * top, tokens), F32),
                vm((d, ff), BF16), vm((d, ff), BF16), vm((ff, d), BF16),
                vm((d, ff), F32), vm((d, ff), F32), vm((ff, d), F32),
                vm((2, rows, d), BF16), vm((2, rows, ff), BF16), vm((2, rows, ff), BF16),
                vm((rows, d), BF16), vm((rows, 2 * ff), BF16),
                vm((2, ep_size, capacity, half), BF16),
                vm((2, side * row_len, capacity, half), BF16),
                vm((row_len * capacity, tokens), BF16),
                vm((top, tokens), jnp.int32), vm((top, tokens), jnp.int32),
                vm((2, chunk, top, d), BF16), vm((tokens, 128), F32),
                vm((2, side - 1, tokens, half), F32), vm((2, tokens, half), F32),
                vm((2, 2, tokens, half), F32), vm((2, 2, tokens // 2, half), F32),
                dma((5,)), dma((3,)), dma((2,)), dma((2, 3)), dma((3,)),
                dma, dma((side * side, 2, 2)), dma((side * side, 2, 2)),
                dma, dma((side * side, 2)), dma((side * side, 2)),
                dma, dma((2, side * row_len)),
                dma, dma((2, 2, 2)), dma((2, 2)),
            ],
            compiler_params=pltpu.CompilerParams(collective_id=0, has_side_effects=True, vmem_limit_bytes=67043328),
            name='moe_bwd',
        )(dy, topk_idx.T, slot_idx.T, gates.T, y_back, x_disp[0], h1_disp[0], h3_disp[0], w_gate[0], w_up[0], w_down[0])
        return dx, d_gates.T, dw1[None], dw3[None], dw2[None]

    return jax.shard_map(
        device_step, mesh=mesh,
        in_specs=(tok_spec, tok_spec, tok_spec, tok_spec, buf_spec, buf_spec, buf_spec, buf_spec,
                  expert_spec, expert_spec, expert_spec),
        out_specs=(tok_spec, tok_spec, buf_spec, buf_spec, buf_spec),
        check_vma=False)
```

```python
import functools
import math

import jax
import jax.numpy as jnp
from jax import lax
from jax.experimental import pallas as pl
from jax.experimental.pallas import tpu as pltpu
from jax.sharding import PartitionSpec as P

F32 = jnp.float32
BF16 = jnp.bfloat16

ORDER = ((0, 0), (1, 0), (3, 0), (0, 1), (0, 3), (2, 0), (0, 2),
         (1, 1), (3, 3), (1, 3), (3, 1), (2, 2), (2, 1), (1, 2), (2, 3), (3, 2))
SENDS = ((0, 1, 2, 3, 4, 5, 6, 7, 8, 9, 10, 11, 12, 13, 14, 15)+(-1,)*8, (-1,)*24)
SUMS = ((9, 0, 0), (10, 1, 0), (16, 1, 2), (17, 0, 2), (18, 1, 1), (19, 0, 1), (20, 1, 3), (21, 0, 3))
JOINS = ((22, 1), (23, 0))
GROUPS = ((1, 'first_near'), (1, 'gates'), (1, 'second_near', 0), (3, 'first_far'), (4, 'second_near', -1),
          (5, 'second_far', 0), (5, 'second_near', 1), (7, 'second_near', 2), (9, 'second_far', -1),
          (10, 'second_far', 1), (11, 'second_far', 2))
STEPS = 24


def mm(a, b, dims):
    return lax.dot_general(a, b, (dims, ((), ())), preferred_element_type=F32)


def pick(k, values):
    out = jnp.int32(values[0])
    for i, v in enumerate(values[1:], 1):
        out = jnp.where(k == i, jnp.int32(v), out)
    return out


def kernel_body(side, capacity, dy_ref, topk_ref, slot_ref, gates_ref, yb_ref, x_ref, h1_ref, h3_ref, w1_ref, w3_ref, w2_ref,
                dx_ref, dg_ref, dw1, dw3, dw2,
                dyall, tab, w1, w3, w2, xb, h1b, h3b, dyd, dh, dxs, rcv, hitb, topk, slots, yb, dg,
                psend, pown, precv, prelay,
                load_sem, w_sem, yb_sem, in_sem, ag_send, ag_recv, ag_recv2, tb_send, tb_recv, tb_recv2,
                r_send, r_recv, p_send, p_recv, pl_recv):
    tokens = dyall.shape[2]
    top = tab.shape[1] // 2
    half = dyall.shape[3]
    ff = h1b.shape[2]
    rows = 2 * capacity
    piece = tokens // 2
    row_len = 2 * side
    me = lax.axis_index('ep')
    core = me % 2
    x = (me // 2) % side
    y = me // (2 * side)
    far = side // 2

    def wrap(v):
        return (v + side) % side

    def block(bx, by):
        return by * side + bx

    def device(bx, by, c):
        return {'ep': block(bx, by) * 2 + c}

    def chip(f, r1, r2):
        return (wrap(x + r1), wrap(y + r2)) if f == 0 else (wrap(x + r2), wrap(y + r1))

    loads = [pltpu.make_async_copy(dy_ref.at[:, pl.ds(f * half, half)], dyall.at[me, f], load_sem.at[f]) for f in (0, 1)]
    loads += [pltpu.make_async_copy(a, b, load_sem.at[2 + i]) for i, (a, b) in enumerate((
        (topk_ref, topk), (slot_ref, slots), (gates_ref, tab.at[me, pl.ds(top, top)])))]
    wloads = [pltpu.make_async_copy(a, b, w_sem.at[i]) for i, (a, b) in enumerate(((w1_ref, w1), (w3_ref, w3), (w2_ref, w2)))]
    for cp in loads + wloads:
        cp.start()

    chunk = yb.shape[1]
    yb_loads = [pltpu.make_async_copy(yb_ref.at[pl.ds(i * chunk, chunk)], yb.at[i % 2], yb_sem.at[i % 2])
                for i in range(tokens // chunk)]
    for cp in yb_loads[:2]:
        cp.start()

    def stream(k):
        b = block(wrap(x + pick(k, [o[0] for o in ORDER])), wrap(y + pick(k, [o[1] for o in ORDER])))
        s = k % 2
        src = pl.ds(b * rows, rows)
        return [pltpu.make_async_copy(x_ref.at[src], xb.at[s], in_sem.at[s, 0]),
                pltpu.make_async_copy(h1_ref.at[src], h1b.at[s], in_sem.at[s, 1]),
                pltpu.make_async_copy(h3_ref.at[src], h3b.at[s], in_sem.at[s, 2])]

    for cp in stream(jnp.int32(0)):
        cp.start()

    barrier = pltpu.get_barrier_semaphore()
    peers = [(wrap(x + r), y) for r in range(1, side)] + [(x, wrap(y + r)) for r in range(1, side)]
    for c in (0, 1):
        for bx, by in peers:
            pl.semaphore_signal(barrier, inc=1, device_id=device(bx, by, c))
    pl.semaphore_signal(barrier, inc=1, device_id=device(x, y, 1 - core))
    for cp in loads:
        cp.wait()
    tab[me, 0:top, :] = jnp.where(slots[...] >= 0, topk[...] * capacity + slots[...], -1).astype(F32)
    pl.semaphore_wait(barrier, 2 * len(peers) + 1)

    def gather_copy(f, p, r1, r2, axis, sign):
        bx, by = chip(f, r1, r2)
        home = block(bx, by) * 2 + core
        src = dyall.at[home, f, pl.ds(p * piece, piece)]
        if axis is None:
            dev, rs, ts = device(x, y, 1 - core), ag_recv2, tb_recv2
        else:
            nx, ny = chip(f, sign, 0) if axis == 0 else chip(f, 0, sign)
            dev, rs, ts = device(nx, ny, core), ag_recv, tb_recv
        out = [pltpu.make_async_remote_copy(src, src, ag_send, rs.at[block(bx, by), f, p], device_id=dev)]
        if f == 0:
            t = tab.at[home, pl.ds(p * top, top)]
            out.append(pltpu.make_async_remote_copy(t, t, tb_send, ts.at[block(bx, by), p], device_id=dev))
        return out

    def send(f, p, r1, r2, axis, sign=0):
        for cp in gather_copy(f, p, r1, r2, axis, sign):
            cp.start()

    def arrived(f, p, r1, r2):
        for cp in gather_copy(f, p, r1, r2, 0, 1):
            cp.wait_recv()

    for axis in (0, 1):
        for f in (0, 1):
            for p, sign in ((0, 1), (1, -1), (1, 1), (0, -1)):
                send(f, p, 0, 0, axis, sign)
    for f in (0, 1):
        for p in (0, 1):
            send(f, p, 0, 0, None)

    def second_axis(f, p, r1):
        send(f, p, r1, 0, 1, 1)
        send(f, p, r1, 0, 1, -1)
        send(f, p, r1, 0, None)

    def first_near():
        for f in (0, 1):
            for p, r in ((0, -1), (1, 1)):
                arrived(f, p, r, 0)
                send(f, p, r, 0, 0, -r)
                second_axis(f, p, r)
        for f in (0, 1):
            for p, r in ((1, -1), (0, 1)):
                arrived(f, p, r, 0)
                second_axis(f, p, r)

    def first_far():
        for f in (0, 1):
            for p in (0, 1):
                arrived(f, p, far, 0)
                second_axis(f, p, far)

    def second_near(r1):
        for f in (0, 1):
            for p, r in ((0, -1), (1, 1)):
                arrived(f, p, r1, r)
                send(f, p, r1, r, 1, -r)
                send(f, p, r1, r, None)
        for f in (0, 1):
            for p, r in ((1, -1), (0, 1)):
                arrived(f, p, r1, r)
                send(f, p, r1, r, None)

    def second_far(r1):
        for f in (0, 1):
            for p in (0, 1):
                arrived(f, p, r1, far)
                send(f, p, r1, far, None)

    def gate_grads(i):
        yb_loads[i].wait()
        part = sum(jnp.sum(dyall[me, f, i * chunk:(i + 1) * chunk, :].astype(F32)[:, None, :]
                           * yb[i % 2, :, :, f * half:(f + 1) * half].astype(F32), axis=2) for f in (0, 1))
        dg[i * chunk:(i + 1) * chunk, 0:top] = part
        if i + 2 < len(yb_loads):
            yb_loads[i + 2].start()

    def gate_grads():
        for i, load in enumerate(yb_loads):
            load.wait()
            part = sum(jnp.sum(dyall[me, f, i * chunk:(i + 1) * chunk, :].astype(F32)[:, None, :]
                               * yb[i % 2, :, :, f * half:(f + 1) * half].astype(F32), axis=2) for f in (0, 1))
            dg[i * chunk:(i + 1) * chunk, 0:top] = part
            if i + 2 < len(yb_loads):
                yb_loads[i + 2].start()
        dg_ref[...] = dg[...].T[0:top, :]

    run = {'first_near': first_near, 'first_far': first_far, 'second_near': second_near,
           'second_far': second_far, 'gates': gate_grads}

    dw1[...] = jnp.zeros_like(dw1)
    dw3[...] = jnp.zeros_like(dw3)
    dw2[...] = jnp.zeros_like(dw2)
    dg[...] = jnp.zeros_like(dg)

    def plane(b):
        home = b * 2 + 1 - core
        for f in (0, 1):
            for p in (0, 1):
                src = dyall.at[home, f, pl.ds(p * piece, piece)]
                pltpu.make_async_copy(src, src, ag_recv2.at[b, f, p]).wait()
        for p in (0, 1):
            t = tab.at[home, pl.ds(p * top, top)]
            pltpu.make_async_copy(t, t, tb_recv2.at[b, p]).wait()

    for cp in wloads:
        cp.wait()

    def compute(k, bx, by):
        s = k % 2
        plane(block(bx, by))
        for cp in stream(k):
            cp.wait()

        @pl.when(k + 1 < len(ORDER))
        def _():
            for cp in stream(k + 1):
                cp.start()

        slot_row = lax.broadcasted_iota(jnp.int32, (capacity, tokens), 0).astype(F32)
        base = (me * capacity).astype(F32)
        for i in (0, 1):
            home = block(bx, by) * 2 + i
            rel = tab[home, 0:top, :] - base
            mine = (rel >= 0.0) & (rel < float(capacity))
            slot = jnp.max(jnp.where(mine, rel, -1.0), axis=0, keepdims=True)
            gate = jnp.sum(jnp.where(mine, tab[home, top:2 * top, :], 0.0), axis=0, keepdims=True)
            hit = slot_row == slot
            row_gate = jnp.sum(jnp.where(hit, gate, 0.0), axis=1, keepdims=True)
            hit = jnp.where(hit, 1.0, 0.0).astype(BF16)
            for f in (0, 1):
                picked = mm(hit, dyall[home, f], ((1,), (0,)))
                dyd[i * capacity:(i + 1) * capacity, f * half:(f + 1) * half] = (row_gate * picked).astype(BF16)
        dyv = dyd[...]
        d_act = mm(dyv, w2[...], ((1,), (1,))).astype(BF16).astype(F32)
        g = h1b[s].astype(F32)
        u = h3b[s].astype(F32)
        sg = jax.nn.sigmoid(g)
        silu = g * sg
        act = (silu * u).astype(BF16)
        dh[:, 0:ff] = (d_act * u * sg * (1.0 + g * (1.0 - sg))).astype(BF16)
        dh[:, ff:2 * ff] = (d_act * silu).astype(BF16)
        dh1 = dh[:, 0:ff]
        dh3 = dh[:, ff:2 * ff]
        for f in (0, 1):
            cols = pl.ds(f * half, half)
            d_x = (mm(dh1, w1[cols, :], ((1,), (1,))) + mm(dh3, w3[cols, :], ((1,), (1,)))).astype(BF16)
            for i in (0, 1):
                dxs[f, block(bx, by) * 2 + i] = d_x[i * capacity:(i + 1) * capacity, :]
        dw2[...] += mm(act, dyv, ((0,), (0,)))
        dw1[...] += mm(xb[s], dh1, ((0,), (0,)))
        dw3[...] += mm(xb[s], dh3, ((0,), (0,)))

    def target(f, sign, c):
        return device(wrap(x + sign), y, c) if f == 0 else device(x, wrap(y + sign), c)

    def send_rows(k):
        bx = wrap(x + pick(k, [o[0] for o in ORDER]))
        by = wrap(y + pick(k, [o[1] for o in ORDER]))
        for f in (0, 1):
            d = pick(k, [o[f] for o in ORDER])
            pos = x if f == 0 else y
            other = by if f == 0 else bx
            slot = other * row_len + pos * 2 + core
            for cc in (0, 1):
                home = block(bx, by) * 2 + cc
                local = (d == 0) & (core == cc)

                @pl.when(local)
                def _():
                    rcv[f, slot] = dxs[f, home]

                @pl.when(jnp.logical_not(local))
                def _():
                    pltpu.make_async_remote_copy(dxs.at[f, home], rcv.at[f, slot], r_send, r_recv.at[f, slot],
                                                 device_id=target(f, d, cc)).start()

    def sums(f, d):
        pos = x if f == 0 else y
        hx, hy = (x, wrap(y + d)) if f == 0 else (wrap(x + d), y)
        other = hy if f == 0 else hx
        home = block(hx, hy) * 2 + core
        code = tab[home, 0:top, :]
        slot_row = lax.broadcasted_iota(jnp.int32, (capacity, tokens), 0).astype(F32)
        for s in range(row_len):
            @pl.when(pos * 2 + core != s)
            def _():
                ref = rcv.at[f, other * row_len + s]
                pltpu.make_async_copy(ref, ref, r_recv.at[f, other * row_len + s]).wait()

            e = y * row_len + s if f == 0 else ((s // 2) * side + x) * 2 + s % 2
            rel = code - (e * capacity).astype(F32)
            slot = jnp.max(jnp.where((rel >= 0.0) & (rel < float(capacity)), rel, -1.0), axis=0, keepdims=True)
            hitb[s * capacity:(s + 1) * capacity, :] = jnp.where(slot_row == slot, 1.0, 0.0).astype(BF16)
        data = rcv[f, pl.ds(other * row_len, row_len)].reshape(row_len * capacity, half)
        return mm(hitb[...], data, ((0,), (0,)))

    def send_sums(f, d, total):
        axis = 1 - f
        if d == far:
            psend[f, d - 1] = total
            for i, sign in ((0, 1), (1, -1)):
                pltpu.make_async_remote_copy(psend.at[f, d - 1, pl.ds(i * piece, piece)], prelay.at[f, i], p_send,
                                             pl_recv.at[f, i], device_id=target(axis, sign, core)).start()
        else:
            i, sign = (0, 1) if d == 1 else (1, -1)
            psend[f, d - 1] = total
            part = pl.ds((1 - i) * piece, piece)
            pltpu.make_async_remote_copy(psend.at[f, d - 1, part], precv.at[f, i, part], p_send, p_recv.at[f, i, 1 - i],
                                         device_id=target(axis, sign, core)).start()

    def join_sums(f):
        for i, sign, d in ((0, 1, 1), (1, -1, side - 1)):
            src = prelay.at[f, i]
            pltpu.make_async_copy(src, src, pl_recv.at[f, i]).wait()
            part = pl.ds(i * piece, piece)
            psend[f, d - 1, part] = psend[f, d - 1, part] + prelay[f, i]
            pltpu.make_async_remote_copy(psend.at[f, d - 1, part], precv.at[f, i, part], p_send, p_recv.at[f, i, i],
                                         device_id=target(1 - f, sign, core)).start()

    def step(k, carry):
        for at, name, *arg in GROUPS:
            @pl.when(k == at)
            def _():
                run[name](*arg)

        @pl.when(k < len(ORDER))
        def _():
            bx = wrap(x + pick(k, [o[0] for o in ORDER]))
            by = wrap(y + pick(k, [o[1] for o in ORDER]))
            compute(k, bx, by)

        for sends in SENDS:
            which = pick(k, sends)

            @pl.when(which >= 0)
            def _():
                send_rows(which)

        for at, f, d in SUMS:
            @pl.when(k == at)
            def _():
                total = sums(f, d)
                if d == 0:
                    pown[f] = total
                else:
                    send_sums(f, d, total)

        for at, f in JOINS:
            @pl.when(k == at)
            def _():
                join_sums(f)

        return carry

    lax.fori_loop(0, STEPS, step, 0)

    for f in (0, 1):
        total = pown[f]
        for i in (0, 1):
            for p in (0, 1):
                ref = precv.at[f, i, pl.ds(p * piece, piece)]
                pltpu.make_async_copy(ref, ref, p_recv.at[f, i, p]).wait()
            total = total + precv[f, i]
        dx_ref[:, f * half:(f + 1) * half] = total.astype(BF16)

    def drained(ref, sem):
        pltpu.make_async_copy(ref, ref, sem).wait()

    chips = side * side
    drained(dyall.at[pl.ds(0, 2 * chips - 1)], ag_send)
    drained(tab.at[pl.ds(0, 2 * chips - 1)], tb_send)
    drained(dxs.at[:, pl.ds(0, 2 * chips - side)], r_send)
    drained(psend, p_send)


def solution(mesh):
    ep_size = mesh.shape['ep']
    side = math.isqrt(ep_size // 2)
    tok_spec = P(('dp', 'ep'), None)
    buf_spec = P(('dp', 'ep'), None, None)
    expert_spec = P('ep', None, None)

    def device_step(dy, topk_idx, slot_idx, gates, y_back, x_disp, h1_disp, h3_disp, w_gate, w_up, w_down):
        capacity = x_disp.shape[1] // ep_size
        tokens, d = dy.shape
        top = gates.shape[1]
        ff = w_gate.shape[2]
        half = d // 2
        rows = 2 * capacity
        row_len = 2 * side

        chunk = tokens // 8
        vm = pltpu.VMEM
        dma = pltpu.SemaphoreType.DMA
        any_spec = pl.BlockSpec(memory_space=pl.ANY)
        dx, d_gates, dw1, dw3, dw2 = pl.pallas_call(
            functools.partial(kernel_body, side, capacity),
            in_specs=[any_spec] * 11,
            out_specs=[pl.BlockSpec(memory_space=pltpu.VMEM)] * 5,
            out_shape=[vm((tokens, d), BF16), vm((top, tokens), F32),
                       vm((d, ff), F32), vm((d, ff), F32), vm((ff, d), F32)],
            scratch_shapes=[
                vm((ep_size, 2, tokens, half), BF16), vm((ep_size, 2 * top, tokens), F32),
                vm((d, ff), BF16), vm((d, ff), BF16), vm((ff, d), BF16),
                vm((2, rows, d), BF16), vm((2, rows, ff), BF16), vm((2, rows, ff), BF16),
                vm((rows, d), BF16), vm((rows, 2 * ff), BF16),
                vm((2, ep_size, capacity, half), BF16),
                vm((2, side * row_len, capacity, half), BF16),
                vm((row_len * capacity, tokens), BF16),
                vm((top, tokens), jnp.int32), vm((top, tokens), jnp.int32),
                vm((2, chunk, top, d), BF16), vm((tokens, 128), F32),
                vm((2, side - 1, tokens, half), F32), vm((2, tokens, half), F32),
                vm((2, 2, tokens, half), F32), vm((2, 2, tokens // 2, half), F32),
                dma((5,)), dma((3,)), dma((2,)), dma((2, 3)),
                dma, dma((side * side, 2, 2)), dma((side * side, 2, 2)),
                dma, dma((side * side, 2)), dma((side * side, 2)),
                dma, dma((2, side * row_len)),
                dma, dma((2, 2, 2)), dma((2, 2)),
            ],
            compiler_params=pltpu.CompilerParams(collective_id=0, has_side_effects=True, vmem_limit_bytes=56 * 2 ** 20),
            name='moe_bwd',
        )(dy, topk_idx.T, slot_idx.T, gates.T, y_back, x_disp[0], h1_disp[0], h3_disp[0], w_gate[0], w_up[0], w_down[0])
        return dx, d_gates.T, dw1[None], dw3[None], dw2[None]

    return jax.shard_map(
        device_step, mesh=mesh,
        in_specs=(tok_spec, tok_spec, tok_spec, tok_spec, buf_spec, buf_spec, buf_spec, buf_spec,
                  expert_spec, expert_spec, expert_spec),
        out_specs=(tok_spec, tok_spec, buf_spec, buf_spec, buf_spec),
        check_vma=False)
```

```python
import functools
import math

import jax
import jax.numpy as jnp
from jax import lax
from jax.experimental import pallas as pl
from jax.experimental.pallas import tpu as pltpu
from jax.sharding import PartitionSpec as P

F32 = jnp.float32
BF16 = jnp.bfloat16

ORDER = ((0, 0), (1, 0), (3, 0), (0, 1), (0, 3), (2, 0), (0, 2),
         (1, 1), (3, 3), (1, 3), (3, 1), (2, 2), (2, 1), (1, 2), (2, 3), (3, 2))
SENDS = ((0, 1, 2, 3, 4, 5, 6, 7, 8, 9, 10, 11, 12, 13, 14, 15)+(-1,)*8, (-1,)*24)
SUMS = ((9, 0, 0), (10, 1, 0), (16, 1, 2), (17, 0, 2), (18, 1, 1), (19, 0, 1), (20, 1, 3), (21, 0, 3))
JOINS = ((22, 1), (23, 0))
GROUPS = ((1, 'first_near'), (1, 'gates'), (1, 'second_near', 0), (3, 'first_far'), (4, 'second_near', -1),
          (5, 'second_far', 0), (5, 'second_near', 1), (7, 'second_near', 2), (9, 'second_far', -1),
          (10, 'second_far', 1), (11, 'second_far', 2))
STEPS = 24


def mm(a, b, dims):
    return lax.dot_general(a, b, (dims, ((), ())), preferred_element_type=F32)


def pick(k, values):
    out = jnp.int32(values[0])
    for i, v in enumerate(values[1:], 1):
        out = jnp.where(k == i, jnp.int32(v), out)
    return out


def kernel_body(side, capacity, dy_ref, topk_ref, slot_ref, gates_ref, yb_ref, x_ref, h1_ref, h3_ref, w1_ref, w3_ref, w2_ref,
                dx_ref, dg_ref, dw1, dw3, dw2,
                dyall, tab, w1, w3, w2, xb, h1b, h3b, dyd, dh, dxs, rcv, hitb, topk, slots, yb, dg,
                psend, pown, precv, prelay,
                load_sem, w_sem, yb_sem, in_sem, ag_send, ag_recv, ag_recv2, tb_send, tb_recv, tb_recv2,
                r_send, r_recv, p_send, p_recv, pl_recv):
    tokens = dyall.shape[2]
    top = tab.shape[1] // 2
    half = dyall.shape[3]
    ff = h1b.shape[2]
    rows = 2 * capacity
    piece = tokens // 2
    row_len = 2 * side
    me = lax.axis_index('ep')
    core = me % 2
    x = (me // 2) % side
    y = me // (2 * side)
    far = side // 2

    def wrap(v):
        return (v + side) % side

    def block(bx, by):
        return by * side + bx

    def device(bx, by, c):
        return {'ep': block(bx, by) * 2 + c}

    def chip(f, r1, r2):
        return (wrap(x + r1), wrap(y + r2)) if f == 0 else (wrap(x + r2), wrap(y + r1))

    loads = [pltpu.make_async_copy(dy_ref.at[:, pl.ds(f * half, half)], dyall.at[me, f], load_sem.at[f]) for f in (0, 1)]
    loads += [pltpu.make_async_copy(a, b, load_sem.at[2 + i]) for i, (a, b) in enumerate((
        (topk_ref, topk), (slot_ref, slots), (gates_ref, tab.at[me, pl.ds(top, top)])))]
    wloads = [pltpu.make_async_copy(a, b, w_sem.at[i]) for i, (a, b) in enumerate(((w1_ref, w1), (w3_ref, w3), (w2_ref, w2)))]
    for cp in loads + wloads:
        cp.start()

    chunk = yb.shape[1]
    yb_loads = [pltpu.make_async_copy(yb_ref.at[pl.ds(i * chunk, chunk)], yb.at[i % 2], yb_sem.at[i % 2])
                for i in range(tokens // chunk)]
    for cp in yb_loads[:2]:
        cp.start()

    def stream(k):
        b = block(wrap(x + pick(k, [o[0] for o in ORDER])), wrap(y + pick(k, [o[1] for o in ORDER])))
        s = k % 2
        src = pl.ds(b * rows, rows)
        return [pltpu.make_async_copy(x_ref.at[src], xb.at[s], in_sem.at[s, 0]),
                pltpu.make_async_copy(h1_ref.at[src], h1b.at[s], in_sem.at[s, 1]),
                pltpu.make_async_copy(h3_ref.at[src], h3b.at[s], in_sem.at[s, 2])]

    for cp in stream(jnp.int32(0)):
        cp.start()

    barrier = pltpu.get_barrier_semaphore()
    peers = [(wrap(x + r), y) for r in range(1, side)] + [(x, wrap(y + r)) for r in range(1, side)]
    for c in (0, 1):
        for bx, by in peers:
            pl.semaphore_signal(barrier, inc=1, device_id=device(bx, by, c))
    pl.semaphore_signal(barrier, inc=1, device_id=device(x, y, 1 - core))
    for cp in loads:
        cp.wait()
    tab[me, 0:top, :] = jnp.where(slots[...] >= 0, topk[...] * capacity + slots[...], -1).astype(F32)
    pl.semaphore_wait(barrier, 2 * len(peers) + 1)

    def gather_copy(f, p, r1, r2, axis, sign):
        bx, by = chip(f, r1, r2)
        home = block(bx, by) * 2 + core
        src = dyall.at[home, f, pl.ds(p * piece, piece)]
        if axis is None:
            dev, rs, ts = device(x, y, 1 - core), ag_recv2, tb_recv2
        else:
            nx, ny = chip(f, sign, 0) if axis == 0 else chip(f, 0, sign)
            dev, rs, ts = device(nx, ny, core), ag_recv, tb_recv
        out = [pltpu.make_async_remote_copy(src, src, ag_send, rs.at[block(bx, by), f, p], device_id=dev)]
        if f == 0:
            t = tab.at[home, pl.ds(p * top, top)]
            out.append(pltpu.make_async_remote_copy(t, t, tb_send, ts.at[block(bx, by), p], device_id=dev))
        return out

    def send(f, p, r1, r2, axis, sign=0):
        for cp in gather_copy(f, p, r1, r2, axis, sign):
            cp.start()

    def arrived(f, p, r1, r2):
        for cp in gather_copy(f, p, r1, r2, 0, 1):
            cp.wait_recv()

    for axis in (0, 1):
        for f in (0, 1):
            for p, sign in ((0, 1), (1, -1), (1, 1), (0, -1)):
                send(f, p, 0, 0, axis, sign)
    for f in (0, 1):
        for p in (0, 1):
            send(f, p, 0, 0, None)

    def second_axis(f, p, r1):
        send(f, p, r1, 0, 1, 1)
        send(f, p, r1, 0, 1, -1)
        send(f, p, r1, 0, None)

    def first_near():
        for f in (0, 1):
            for p, r in ((0, -1), (1, 1)):
                arrived(f, p, r, 0)
                send(f, p, r, 0, 0, -r)
                second_axis(f, p, r)
        for f in (0, 1):
            for p, r in ((1, -1), (0, 1)):
                arrived(f, p, r, 0)
                second_axis(f, p, r)

    def first_far():
        for f in (0, 1):
            for p in (0, 1):
                arrived(f, p, far, 0)
                second_axis(f, p, far)

    def second_near(r1):
        for f in (0, 1):
            for p, r in ((0, -1), (1, 1)):
                arrived(f, p, r1, r)
                send(f, p, r1, r, 1, -r)
                send(f, p, r1, r, None)
        for f in (0, 1):
            for p, r in ((1, -1), (0, 1)):
                arrived(f, p, r1, r)
                send(f, p, r1, r, None)

    def second_far(r1):
        for f in (0, 1):
            for p in (0, 1):
                arrived(f, p, r1, far)
                send(f, p, r1, far, None)

    def gate_grads(i):
        yb_loads[i].wait()
        part = sum(jnp.sum(dyall[me, f, i * chunk:(i + 1) * chunk, :].astype(F32)[:, None, :]
                           * yb[i % 2, :, :, f * half:(f + 1) * half].astype(F32), axis=2) for f in (0, 1))
        dg[i * chunk:(i + 1) * chunk, 0:top] = part
        if i + 2 < len(yb_loads):
            yb_loads[i + 2].start()

    def gate_grads():
        for i, load in enumerate(yb_loads):
            load.wait()
            part = sum(jnp.sum(dyall[me, f, i * chunk:(i + 1) * chunk, :].astype(F32)[:, None, :]
                               * yb[i % 2, :, :, f * half:(f + 1) * half].astype(F32), axis=2) for f in (0, 1))
            dg[i * chunk:(i + 1) * chunk, 0:top] = part
            if i + 2 < len(yb_loads):
                yb_loads[i + 2].start()
        dg_ref[...] = dg[...].T[0:top, :]

    run = {'first_near': first_near, 'first_far': first_far, 'second_near': second_near,
           'second_far': second_far, 'gates': gate_grads}

    dw1[...] = jnp.zeros_like(dw1)
    dw3[...] = jnp.zeros_like(dw3)
    dw2[...] = jnp.zeros_like(dw2)
    dg[...] = jnp.zeros_like(dg)

    def plane(b):
        home = b * 2 + 1 - core
        for f in (0, 1):
            for p in (0, 1):
                src = dyall.at[home, f, pl.ds(p * piece, piece)]
                pltpu.make_async_copy(src, src, ag_recv2.at[b, f, p]).wait()
        for p in (0, 1):
            t = tab.at[home, pl.ds(p * top, top)]
            pltpu.make_async_copy(t, t, tb_recv2.at[b, p]).wait()

    for cp in wloads:
        cp.wait()

    def compute(k, bx, by):
        s = k % 2
        plane(block(bx, by))
        for cp in stream(k):
            cp.wait()

        @pl.when(k + 1 < len(ORDER))
        def _():
            for cp in stream(k + 1):
                cp.start()

        slot_row = lax.broadcasted_iota(jnp.int32, (capacity, tokens), 0).astype(F32)
        base = (me * capacity).astype(F32)
        for i in (0, 1):
            home = block(bx, by) * 2 + i
            rel = tab[home, 0:top, :] - base
            mine = (rel >= 0.0) & (rel < float(capacity))
            slot = jnp.max(jnp.where(mine, rel, -1.0), axis=0, keepdims=True)
            gate = jnp.sum(jnp.where(mine, tab[home, top:2 * top, :], 0.0), axis=0, keepdims=True)
            hit = slot_row == slot
            row_gate = jnp.sum(jnp.where(hit, gate, 0.0), axis=1, keepdims=True)
            hit = jnp.where(hit, 1.0, 0.0).astype(BF16)
            for f in (0, 1):
                picked = mm(hit, dyall[home, f], ((1,), (0,)))
                dyd[i * capacity:(i + 1) * capacity, f * half:(f + 1) * half] = (row_gate * picked).astype(BF16)
        dyv = dyd[...]
        d_act = mm(dyv, w2[...], ((1,), (1,))).astype(BF16).astype(F32)
        g = h1b[s].astype(F32)
        u = h3b[s].astype(F32)
        sg = jax.nn.sigmoid(g)
        silu = g * sg
        act = (silu * u).astype(BF16)
        dh[:, 0:ff] = (d_act * u * sg * (1.0 + g * (1.0 - sg))).astype(BF16)
        dh[:, ff:2 * ff] = (d_act * silu).astype(BF16)
        dh1 = dh[:, 0:ff]
        dh3 = dh[:, ff:2 * ff]
        for f in (0, 1):
            cols = pl.ds(f * half, half)
            d_x = (mm(dh1, w1[cols, :], ((1,), (1,))) + mm(dh3, w3[cols, :], ((1,), (1,)))).astype(BF16)
            for i in (0, 1):
                dxs[f, block(bx, by) * 2 + i] = d_x[i * capacity:(i + 1) * capacity, :]
        dw2[...] += mm(act, dyv, ((0,), (0,)))
        dw1[...] += mm(xb[s], dh1, ((0,), (0,)))
        dw3[...] += mm(xb[s], dh3, ((0,), (0,)))

    def target(f, sign, c):
        return device(wrap(x + sign), y, c) if f == 0 else device(x, wrap(y + sign), c)

    def send_rows(k):
        bx = wrap(x + pick(k, [o[0] for o in ORDER]))
        by = wrap(y + pick(k, [o[1] for o in ORDER]))
        for f in (0, 1):
            d = pick(k, [o[f] for o in ORDER])
            pos = x if f == 0 else y
            other = by if f == 0 else bx
            slot = other * row_len + pos * 2 + core
            for cc in (0, 1):
                home = block(bx, by) * 2 + cc
                local = (d == 0) & (core == cc)

                @pl.when(local)
                def _():
                    rcv[f, slot] = dxs[f, home]

                @pl.when(jnp.logical_not(local))
                def _():
                    pltpu.make_async_remote_copy(dxs.at[f, home], rcv.at[f, slot], r_send, r_recv.at[f, slot],
                                                 device_id=target(f, d, cc)).start()

    def sums(f, d):
        pos = x if f == 0 else y
        hx, hy = (x, wrap(y + d)) if f == 0 else (wrap(x + d), y)
        other = hy if f == 0 else hx
        home = block(hx, hy) * 2 + core
        code = tab[home].T[:, 0:top]
        slot_col = lax.broadcasted_iota(jnp.int32, (tokens, capacity), 1).astype(F32)
        for s in range(row_len):
            e = y * row_len + s if f == 0 else ((s // 2) * side + x) * 2 + s % 2
            rel = code - (e * capacity).astype(F32)
            slot = jnp.max(jnp.where((rel >= 0.0) & (rel < float(capacity)), rel, -1.0), axis=1, keepdims=True)
            hitb[:, s * capacity:(s + 1) * capacity] = jnp.where(slot_col == slot, 1.0, 0.0).astype(BF16)
        for s in range(row_len):
            @pl.when(pos * 2 + core != s)
            def _():
                ref = rcv.at[f, other * row_len + s]
                pltpu.make_async_copy(ref, ref, r_recv.at[f, other * row_len + s]).wait()

        data = rcv[f, pl.ds(other * row_len, row_len)].reshape(row_len * capacity, half)
        return mm(hitb[...], data, ((1,), (0,)))

    def send_sums(f, d, total):
        axis = 1 - f
        if d == far:
            psend[f, d - 1] = total
            for i, sign in ((0, 1), (1, -1)):
                pltpu.make_async_remote_copy(psend.at[f, d - 1, pl.ds(i * piece, piece)], prelay.at[f, i], p_send,
                                             pl_recv.at[f, i], device_id=target(axis, sign, core)).start()
        else:
            i, sign = (0, 1) if d == 1 else (1, -1)
            psend[f, d - 1] = total
            part = pl.ds((1 - i) * piece, piece)
            pltpu.make_async_remote_copy(psend.at[f, d - 1, part], precv.at[f, i, part], p_send, p_recv.at[f, i, 1 - i],
                                         device_id=target(axis, sign, core)).start()

    def join_sums(f):
        for i, sign, d in ((0, 1, 1), (1, -1, side - 1)):
            src = prelay.at[f, i]
            pltpu.make_async_copy(src, src, pl_recv.at[f, i]).wait()
            part = pl.ds(i * piece, piece)
            psend[f, d - 1, part] = psend[f, d - 1, part] + prelay[f, i]
            pltpu.make_async_remote_copy(psend.at[f, d - 1, part], precv.at[f, i, part], p_send, p_recv.at[f, i, i],
                                         device_id=target(1 - f, sign, core)).start()

    def step(k, carry):
        for at, name, *arg in GROUPS:
            @pl.when(k == at)
            def _():
                run[name](*arg)

        @pl.when(k < len(ORDER))
        def _():
            bx = wrap(x + pick(k, [o[0] for o in ORDER]))
            by = wrap(y + pick(k, [o[1] for o in ORDER]))
            compute(k, bx, by)

        for sends in SENDS:
            which = pick(k, sends)

            @pl.when(which >= 0)
            def _():
                send_rows(which)

        for at, f, d in SUMS:
            @pl.when(k == at)
            def _():
                total = sums(f, d)
                if d == 0:
                    pown[f] = total
                else:
                    send_sums(f, d, total)

        for at, f in JOINS:
            @pl.when(k == at)
            def _():
                join_sums(f)

        return carry

    lax.fori_loop(0, STEPS, step, 0)

    for f in (0, 1):
        total = pown[f]
        for i in (0, 1):
            for p in (0, 1):
                ref = precv.at[f, i, pl.ds(p * piece, piece)]
                pltpu.make_async_copy(ref, ref, p_recv.at[f, i, p]).wait()
            total = total + precv[f, i]
        dx_ref[:, f * half:(f + 1) * half] = total.astype(BF16)

    def drained(ref, sem):
        pltpu.make_async_copy(ref, ref, sem).wait()

    chips = side * side
    drained(dyall.at[pl.ds(0, 2 * chips - 1)], ag_send)
    drained(tab.at[pl.ds(0, 2 * chips - 1)], tb_send)
    drained(dxs.at[:, pl.ds(0, 2 * chips - side)], r_send)
    drained(psend, p_send)


def write_out(*refs):
    n = (len(refs) - 1) // 2
    copies = [pltpu.make_async_copy(refs[i], refs[n + i], refs[-1].at[i]) for i in range(n)]
    for cp in copies:
        cp.start()
    for cp in copies:
        cp.wait()


def solution(mesh):
    ep_size = mesh.shape['ep']
    side = math.isqrt(ep_size // 2)
    tok_spec = P(('dp', 'ep'), None)
    buf_spec = P(('dp', 'ep'), None, None)
    expert_spec = P('ep', None, None)

    def device_step(dy, topk_idx, slot_idx, gates, y_back, x_disp, h1_disp, h3_disp, w_gate, w_up, w_down):
        capacity = x_disp.shape[1] // ep_size
        tokens, d = dy.shape
        top = gates.shape[1]
        ff = w_gate.shape[2]
        half = d // 2
        rows = 2 * capacity
        row_len = 2 * side

        chunk = tokens // 8
        vm = pltpu.VMEM
        dma = pltpu.SemaphoreType.DMA
        any_spec = pl.BlockSpec(memory_space=pl.ANY)
        kept = pl.pallas_call(
            functools.partial(kernel_body, side, capacity),
            in_specs=[any_spec] * 11,
            out_specs=[pl.BlockSpec(memory_space=pltpu.VMEM)] * 5,
            out_shape=[vm((tokens, d), BF16), vm((top, tokens), F32),
                       vm((d, ff), F32), vm((d, ff), F32), vm((ff, d), F32)],
            scratch_shapes=[
                vm((ep_size, 2, tokens, half), BF16), vm((ep_size, 2 * top, tokens), F32),
                vm((d, ff), BF16), vm((d, ff), BF16), vm((ff, d), BF16),
                vm((2, rows, d), BF16), vm((2, rows, ff), BF16), vm((2, rows, ff), BF16),
                vm((rows, d), BF16), vm((rows, 2 * ff), BF16),
                vm((2, ep_size, capacity, half), BF16),
                vm((2, side * row_len, capacity, half), BF16),
                vm((tokens, row_len * capacity), BF16),
                vm((top, tokens), jnp.int32), vm((top, tokens), jnp.int32),
                vm((2, chunk, top, d), BF16), vm((tokens, 128), F32),
                vm((2, side - 1, tokens, half), F32), vm((2, tokens, half), F32),
                vm((2, 2, tokens, half), F32), vm((2, 2, tokens // 2, half), F32),
                dma((5,)), dma((3,)), dma((2,)), dma((2, 3)),
                dma, dma((side * side, 2, 2)), dma((side * side, 2, 2)),
                dma, dma((side * side, 2)), dma((side * side, 2)),
                dma, dma((2, side * row_len)),
                dma, dma((2, 2, 2)), dma((2, 2)),
            ],
            compiler_params=pltpu.CompilerParams(collective_id=0, has_side_effects=True, vmem_limit_bytes=56 * 2 ** 20),
            name='moe_bwd',
        )(dy, topk_idx.T, slot_idx.T, gates.T, y_back, x_disp[0], h1_disp[0], h3_disp[0], w_gate[0], w_up[0], w_down[0])
        dx, d_gates, dw1, dw3, dw2 = pl.pallas_call(
            write_out,
            in_specs=[pl.BlockSpec(memory_space=pltpu.VMEM)] * len(kept),
            out_specs=[any_spec] * len(kept),
            out_shape=[jax.ShapeDtypeStruct(a.shape, a.dtype) for a in kept],
            scratch_shapes=[dma((len(kept),))], name='write_out',
            compiler_params=pltpu.CompilerParams(vmem_limit_bytes=2 ** 20),
        )(*[pltpu.with_memory_space_constraint(a, pltpu.VMEM) for a in kept])
        return dx, d_gates.T, dw1[None], dw3[None], dw2[None]

    return jax.shard_map(
        device_step, mesh=mesh,
        in_specs=(tok_spec, tok_spec, tok_spec, tok_spec, buf_spec, buf_spec, buf_spec, buf_spec,
                  expert_spec, expert_spec, expert_spec),
        out_specs=(tok_spec, tok_spec, buf_spec, buf_spec, buf_spec),
        check_vma=False)
```

```python
import functools
import math

import jax
import jax.numpy as jnp
from jax import lax
from jax.experimental import pallas as pl
from jax.experimental.pallas import tpu as pltpu
from jax.sharding import PartitionSpec as P

F32 = jnp.float32
BF16 = jnp.bfloat16

ORDER = ((0, 0), (1, 0), (3, 0), (0, 1), (0, 3), (2, 0), (0, 2),
         (1, 1), (3, 3), (1, 3), (3, 1), (2, 2), (2, 1), (1, 2), (2, 3), (3, 2))
SENDS = ((0, 1, 2, 3, 4, 5, 6, 7, 8, 9, 10, 11, 12, 13, 14, 15)+(-1,)*8, (-1,)*24)
SUMS = ((9, 0, 0), (10, 1, 0), (16, 1, 2), (17, 0, 2), (18, 1, 1), (19, 0, 1), (20, 1, 3), (21, 0, 3))
JOINS = ((22, 1), (23, 0))
GROUPS = ((1, 'first_near'), (1, 'gates'), (1, 'second_near', 0), (3, 'first_far'), (4, 'second_near', -1),
          (5, 'second_far', 0), (5, 'second_near', 1), (7, 'second_near', 2), (9, 'second_far', -1),
          (10, 'second_far', 1), (11, 'second_far', 2))
STEPS = 24


def mm(a, b, dims):
    return lax.dot_general(a, b, (dims, ((), ())), preferred_element_type=F32)


def pick(k, values):
    out = jnp.int32(values[0])
    for i, v in enumerate(values[1:], 1):
        out = jnp.where(k == i, jnp.int32(v), out)
    return out


def kernel_body(side, capacity, dy_ref, topk_ref, slot_ref, gates_ref, yb_ref, x_ref, h1_ref, h3_ref, w1_ref, w3_ref, w2_ref,
                dx_ref, dg_ref, dw1, dw3, dw2,
                dyall, tab, w1, w3, w2, xb, h1b, h3b, dyd, dh, dxs, rcv, hitb, topk, slots, yb, dg,
                psend, pown, precv, prelay,
                load_sem, w_sem, yb_sem, in_sem, ag_send, ag_recv, ag_recv2, tb_send, tb_recv, tb_recv2,
                r_send, r_recv, p_send, p_recv, pl_recv):
    tokens = dyall.shape[2]
    top = tab.shape[1] // 2
    half = dyall.shape[3]
    ff = h1b.shape[2]
    rows = 2 * capacity
    piece = tokens // 2
    row_len = 2 * side
    me = lax.axis_index('ep')
    core = me % 2
    x = (me // 2) % side
    y = me // (2 * side)
    far = side // 2

    def wrap(v):
        return (v + side) % side

    def block(bx, by):
        return by * side + bx

    def device(bx, by, c):
        return {'ep': block(bx, by) * 2 + c}

    def chip(f, r1, r2):
        return (wrap(x + r1), wrap(y + r2)) if f == 0 else (wrap(x + r2), wrap(y + r1))

    loads = [pltpu.make_async_copy(dy_ref.at[:, pl.ds(f * half, half)], dyall.at[me, f], load_sem.at[f]) for f in (0, 1)]
    loads += [pltpu.make_async_copy(a, b, load_sem.at[2 + i]) for i, (a, b) in enumerate((
        (topk_ref, topk), (slot_ref, slots), (gates_ref, tab.at[me, pl.ds(top, top)])))]
    wloads = [pltpu.make_async_copy(a, b, w_sem.at[i]) for i, (a, b) in enumerate(((w1_ref, w1), (w3_ref, w3), (w2_ref, w2)))]
    for cp in loads + wloads:
        cp.start()

    chunk = yb.shape[1]
    yb_loads = [pltpu.make_async_copy(yb_ref.at[pl.ds(i * chunk, chunk)], yb.at[i % 2], yb_sem.at[i % 2])
                for i in range(tokens // chunk)]
    for cp in yb_loads[:2]:
        cp.start()

    def stream(k):
        b = block(wrap(x + pick(k, [o[0] for o in ORDER])), wrap(y + pick(k, [o[1] for o in ORDER])))
        s = k % 2
        src = pl.ds(b * rows, rows)
        return [pltpu.make_async_copy(x_ref.at[src], xb.at[s], in_sem.at[s, 0]),
                pltpu.make_async_copy(h1_ref.at[src], h1b.at[s], in_sem.at[s, 1]),
                pltpu.make_async_copy(h3_ref.at[src], h3b.at[s], in_sem.at[s, 2])]

    for cp in stream(jnp.int32(0)):
        cp.start()

    barrier = pltpu.get_barrier_semaphore()
    peers = [(wrap(x + 1), y), (wrap(x - 1), y), (x, wrap(y + 1)), (x, wrap(y - 1))]
    for bx, by in peers:
        pl.semaphore_signal(barrier, inc=1, device_id=device(bx, by, core))
    pl.semaphore_signal(barrier, inc=1, device_id=device(x, y, 1 - core))
    for cp in loads:
        cp.wait()
    tab[me, 0:top, :] = jnp.where(slots[...] >= 0, topk[...] * capacity + slots[...], -1).astype(F32)
    pl.semaphore_wait(barrier, len(peers) + 1)

    def gather_copy(f, p, r1, r2, axis, sign):
        bx, by = chip(f, r1, r2)
        home = block(bx, by) * 2 + core
        src = dyall.at[home, f, pl.ds(p * piece, piece)]
        if axis is None:
            dev, rs, ts = device(x, y, 1 - core), ag_recv2, tb_recv2
        else:
            nx, ny = chip(f, sign, 0) if axis == 0 else chip(f, 0, sign)
            dev, rs, ts = device(nx, ny, core), ag_recv, tb_recv
        out = [pltpu.make_async_remote_copy(src, src, ag_send, rs.at[block(bx, by), f, p], device_id=dev)]
        if f == p:
            t = tab.at[home, pl.ds(p * top, top)]
            out.append(pltpu.make_async_remote_copy(t, t, tb_send, ts.at[block(bx, by), p], device_id=dev))
        return out

    def send(f, p, r1, r2, axis, sign=0):
        for cp in gather_copy(f, p, r1, r2, axis, sign):
            cp.start()

    def arrived(f, p, r1, r2):
        for cp in gather_copy(f, p, r1, r2, 0, 1):
            cp.wait_recv()

    for axis in (0, 1):
        for f in (0, 1):
            for p, sign in ((0, 1), (1, -1), (1, 1), (0, -1)):
                send(f, p, 0, 0, axis, sign)
    for f in (0, 1):
        for p in (0, 1):
            send(f, p, 0, 0, None)

    def second_axis(f, p, r1):
        send(f, p, r1, 0, 1, 1)
        send(f, p, r1, 0, 1, -1)
        send(f, p, r1, 0, None)

    def first_near():
        for f in (0, 1):
            for p, r in ((0, -1), (1, 1)):
                arrived(f, p, r, 0)
                send(f, p, r, 0, 0, -r)
                second_axis(f, p, r)
        for f in (0, 1):
            for p, r in ((1, -1), (0, 1)):
                arrived(f, p, r, 0)
                second_axis(f, p, r)

    def first_far():
        for f in (0, 1):
            for p in (0, 1):
                arrived(f, p, far, 0)
                second_axis(f, p, far)

    def second_near(r1):
        for f in (0, 1):
            for p, r in ((0, -1), (1, 1)):
                arrived(f, p, r1, r)
                send(f, p, r1, r, 1, -r)
                send(f, p, r1, r, None)
        for f in (0, 1):
            for p, r in ((1, -1), (0, 1)):
                arrived(f, p, r1, r)
                send(f, p, r1, r, None)

    def second_far(r1):
        for f in (0, 1):
            for p in (0, 1):
                arrived(f, p, r1, far)
                send(f, p, r1, far, None)

    def gate_grads(i):
        yb_loads[i].wait()
        part = sum(jnp.sum(dyall[me, f, i * chunk:(i + 1) * chunk, :].astype(F32)[:, None, :]
                           * yb[i % 2, :, :, f * half:(f + 1) * half].astype(F32), axis=2) for f in (0, 1))
        dg[i * chunk:(i + 1) * chunk, 0:top] = part
        if i + 2 < len(yb_loads):
            yb_loads[i + 2].start()

    def gate_grads():
        for i, load in enumerate(yb_loads):
            load.wait()
            part = sum(jnp.sum(dyall[me, f, i * chunk:(i + 1) * chunk, :].astype(F32)[:, None, :]
                               * yb[i % 2, :, :, f * half:(f + 1) * half].astype(F32), axis=2) for f in (0, 1))
            dg[i * chunk:(i + 1) * chunk, 0:top] = part
            if i + 2 < len(yb_loads):
                yb_loads[i + 2].start()
        dg_ref[...] = dg[...].T[0:top, :]

    run = {'first_near': first_near, 'first_far': first_far, 'second_near': second_near,
           'second_far': second_far, 'gates': gate_grads}

    dw1[...] = jnp.zeros_like(dw1)
    dw3[...] = jnp.zeros_like(dw3)
    dw2[...] = jnp.zeros_like(dw2)
    dg[...] = jnp.zeros_like(dg)

    def plane(b):
        home = b * 2 + 1 - core
        for f in (0, 1):
            for p in (0, 1):
                src = dyall.at[home, f, pl.ds(p * piece, piece)]
                pltpu.make_async_copy(src, src, ag_recv2.at[b, f, p]).wait()
        for p in (0, 1):
            t = tab.at[home, pl.ds(p * top, top)]
            pltpu.make_async_copy(t, t, tb_recv2.at[b, p]).wait()

    for cp in wloads:
        cp.wait()

    def compute(k, bx, by):
        s = k % 2
        plane(block(bx, by))
        for cp in stream(k):
            cp.wait()

        @pl.when(k + 1 < len(ORDER))
        def _():
            for cp in stream(k + 1):
                cp.start()

        slot_row = lax.broadcasted_iota(jnp.int32, (capacity, tokens), 0).astype(F32)
        base = (me * capacity).astype(F32)
        for i in (0, 1):
            home = block(bx, by) * 2 + i
            rel = tab[home, 0:top, :] - base
            mine = (rel >= 0.0) & (rel < float(capacity))
            slot = jnp.max(jnp.where(mine, rel, -1.0), axis=0, keepdims=True)
            gate = jnp.sum(jnp.where(mine, tab[home, top:2 * top, :], 0.0), axis=0, keepdims=True)
            hit = slot_row == slot
            row_gate = jnp.sum(jnp.where(hit, gate, 0.0), axis=1, keepdims=True)
            hit = jnp.where(hit, 1.0, 0.0).astype(BF16)
            for f in (0, 1):
                picked = mm(hit, dyall[home, f], ((1,), (0,)))
                dyd[i * capacity:(i + 1) * capacity, f * half:(f + 1) * half] = (row_gate * picked).astype(BF16)
        dyv = dyd[...]
        d_act = mm(dyv, w2[...], ((1,), (1,))).astype(BF16).astype(F32)
        g = h1b[s].astype(F32)
        u = h3b[s].astype(F32)
        sg = jax.nn.sigmoid(g)
        silu = g * sg
        act = (silu * u).astype(BF16)
        dh[:, 0:ff] = (d_act * u * sg * (1.0 + g * (1.0 - sg))).astype(BF16)
        dh[:, ff:2 * ff] = (d_act * silu).astype(BF16)
        dh1 = dh[:, 0:ff]
        dh3 = dh[:, ff:2 * ff]
        for f in (0, 1):
            cols = pl.ds(f * half, half)
            d_x = (mm(dh1, w1[cols, :], ((1,), (1,))) + mm(dh3, w3[cols, :], ((1,), (1,)))).astype(BF16)
            for i in (0, 1):
                dxs[f, block(bx, by) * 2 + i] = d_x[i * capacity:(i + 1) * capacity, :]
        dw2[...] += mm(act, dyv, ((0,), (0,)))
        dw1[...] += mm(xb[s], dh1, ((0,), (0,)))
        dw3[...] += mm(xb[s], dh3, ((0,), (0,)))

    def target(f, sign, c):
        return device(wrap(x + sign), y, c) if f == 0 else device(x, wrap(y + sign), c)

    def send_rows(k):
        bx = wrap(x + pick(k, [o[0] for o in ORDER]))
        by = wrap(y + pick(k, [o[1] for o in ORDER]))
        for f in (0, 1):
            d = pick(k, [o[f] for o in ORDER])
            pos = x if f == 0 else y
            other = by if f == 0 else bx
            slot = other * row_len + pos * 2 + core
            for cc in (0, 1):
                home = block(bx, by) * 2 + cc
                local = (d == 0) & (core == cc)

                @pl.when(local)
                def _():
                    rcv[f, slot] = dxs[f, home]

                @pl.when(jnp.logical_not(local))
                def _():
                    pltpu.make_async_remote_copy(dxs.at[f, home], rcv.at[f, slot], r_send, r_recv.at[f, slot],
                                                 device_id=target(f, d, cc)).start()

    def sums(f, d):
        pos = x if f == 0 else y
        hx, hy = (x, wrap(y + d)) if f == 0 else (wrap(x + d), y)
        other = hy if f == 0 else hx
        home = block(hx, hy) * 2 + core
        code = tab[home].T[:, 0:top]
        slot_col = lax.broadcasted_iota(jnp.int32, (tokens, capacity), 1).astype(F32)
        for s in range(row_len):
            e = y * row_len + s if f == 0 else ((s // 2) * side + x) * 2 + s % 2
            rel = code - (e * capacity).astype(F32)
            slot = jnp.max(jnp.where((rel >= 0.0) & (rel < float(capacity)), rel, -1.0), axis=1, keepdims=True)
            hitb[:, s * capacity:(s + 1) * capacity] = jnp.where(slot_col == slot, 1.0, 0.0).astype(BF16)
        for s in range(row_len):
            @pl.when(pos * 2 + core != s)
            def _():
                ref = rcv.at[f, other * row_len + s]
                pltpu.make_async_copy(ref, ref, r_recv.at[f, other * row_len + s]).wait()

        data = rcv[f, pl.ds(other * row_len, row_len)].reshape(row_len * capacity, half)
        return mm(hitb[...], data, ((1,), (0,)))

    def send_sums(f, d, total):
        axis = 1 - f
        if d == far:
            psend[f, d - 1] = total
            for i, sign in ((0, 1), (1, -1)):
                pltpu.make_async_remote_copy(psend.at[f, d - 1, pl.ds(i * piece, piece)], prelay.at[f, i], p_send,
                                             pl_recv.at[f, i], device_id=target(axis, sign, core)).start()
        else:
            i, sign = (0, 1) if d == 1 else (1, -1)
            psend[f, d - 1] = total
            part = pl.ds((1 - i) * piece, piece)
            pltpu.make_async_remote_copy(psend.at[f, d - 1, part], precv.at[f, i, part], p_send, p_recv.at[f, i, 1 - i],
                                         device_id=target(axis, sign, core)).start()

    def join_sums(f):
        for i, sign, d in ((0, 1, 1), (1, -1, side - 1)):
            src = prelay.at[f, i]
            pltpu.make_async_copy(src, src, pl_recv.at[f, i]).wait()
            part = pl.ds(i * piece, piece)
            psend[f, d - 1, part] = psend[f, d - 1, part] + prelay[f, i]
            pltpu.make_async_remote_copy(psend.at[f, d - 1, part], precv.at[f, i, part], p_send, p_recv.at[f, i, i],
                                         device_id=target(1 - f, sign, core)).start()

    def step(k, carry):
        for at, name, *arg in GROUPS:
            @pl.when(k == at)
            def _():
                run[name](*arg)

        @pl.when(k < len(ORDER))
        def _():
            bx = wrap(x + pick(k, [o[0] for o in ORDER]))
            by = wrap(y + pick(k, [o[1] for o in ORDER]))
            compute(k, bx, by)

        for sends in SENDS:
            which = pick(k, sends)

            @pl.when(which >= 0)
            def _():
                send_rows(which)

        for at, f, d in SUMS:
            @pl.when(k == at)
            def _():
                total = sums(f, d)
                if d == 0:
                    pown[f] = total
                else:
                    send_sums(f, d, total)

        for at, f in JOINS:
            @pl.when(k == at)
            def _():
                join_sums(f)

        return carry

    lax.fori_loop(0, STEPS, step, 0)

    for f in (0, 1):
        total = pown[f]
        for i in (0, 1):
            for p in (0, 1):
                ref = precv.at[f, i, pl.ds(p * piece, piece)]
                pltpu.make_async_copy(ref, ref, p_recv.at[f, i, p]).wait()
            total = total + precv[f, i]
        dx_ref[:, f * half:(f + 1) * half] = total.astype(BF16)

    def drained(ref, sem):
        pltpu.make_async_copy(ref, ref, sem).wait()

    chips = side * side
    drained(dyall.at[pl.ds(0, 2 * chips - 1)], ag_send)
    drained(tab.at[pl.ds(0, 2 * chips - 1)], tb_send)
    drained(dxs.at[:, pl.ds(0, 2 * chips - side)], r_send)
    drained(psend, p_send)


def write_out(*refs):
    n = (len(refs) - 1) // 2
    copies = [pltpu.make_async_copy(refs[i], refs[n + i], refs[-1].at[i]) for i in range(n)]
    for cp in copies:
        cp.start()
    for cp in copies:
        cp.wait()


def solution(mesh):
    ep_size = mesh.shape['ep']
    side = math.isqrt(ep_size // 2)
    tok_spec = P(('dp', 'ep'), None)
    buf_spec = P(('dp', 'ep'), None, None)
    expert_spec = P('ep', None, None)

    def device_step(dy, topk_idx, slot_idx, gates, y_back, x_disp, h1_disp, h3_disp, w_gate, w_up, w_down):
        capacity = x_disp.shape[1] // ep_size
        tokens, d = dy.shape
        top = gates.shape[1]
        ff = w_gate.shape[2]
        half = d // 2
        rows = 2 * capacity
        row_len = 2 * side

        chunk = tokens // 8
        vm = pltpu.VMEM
        dma = pltpu.SemaphoreType.DMA
        any_spec = pl.BlockSpec(memory_space=pl.ANY)
        kept = pl.pallas_call(
            functools.partial(kernel_body, side, capacity),
            in_specs=[any_spec] * 11,
            out_specs=[pl.BlockSpec(memory_space=pltpu.VMEM)] * 5,
            out_shape=[vm((tokens, d), BF16), vm((top, tokens), F32),
                       vm((d, ff), F32), vm((d, ff), F32), vm((ff, d), F32)],
            scratch_shapes=[
                vm((ep_size, 2, tokens, half), BF16), vm((ep_size, 2 * top, tokens), F32),
                vm((d, ff), BF16), vm((d, ff), BF16), vm((ff, d), BF16),
                vm((2, rows, d), BF16), vm((2, rows, ff), BF16), vm((2, rows, ff), BF16),
                vm((rows, d), BF16), vm((rows, 2 * ff), BF16),
                vm((2, ep_size, capacity, half), BF16),
                vm((2, side * row_len, capacity, half), BF16),
                vm((tokens, row_len * capacity), BF16),
                vm((top, tokens), jnp.int32), vm((top, tokens), jnp.int32),
                vm((2, chunk, top, d), BF16), vm((tokens, 128), F32),
                vm((2, side - 1, tokens, half), F32), vm((2, tokens, half), F32),
                vm((2, 2, tokens, half), F32), vm((2, 2, tokens // 2, half), F32),
                dma((5,)), dma((3,)), dma((2,)), dma((2, 3)),
                dma, dma((side * side, 2, 2)), dma((side * side, 2, 2)),
                dma, dma((side * side, 2)), dma((side * side, 2)),
                dma, dma((2, side * row_len)),
                dma, dma((2, 2, 2)), dma((2, 2)),
            ],
            compiler_params=pltpu.CompilerParams(collective_id=0, has_side_effects=True, vmem_limit_bytes=56 * 2 ** 20),
            name='moe_bwd',
        )(dy, topk_idx.T, slot_idx.T, gates.T, y_back, x_disp[0], h1_disp[0], h3_disp[0], w_gate[0], w_up[0], w_down[0])
        dx, d_gates, dw1, dw3, dw2 = pl.pallas_call(
            write_out,
            in_specs=[pl.BlockSpec(memory_space=pltpu.VMEM)] * len(kept),
            out_specs=[any_spec] * len(kept),
            out_shape=[jax.ShapeDtypeStruct(a.shape, a.dtype) for a in kept],
            scratch_shapes=[dma((len(kept),))], name='write_out',
            compiler_params=pltpu.CompilerParams(vmem_limit_bytes=2 ** 20),
        )(*[pltpu.with_memory_space_constraint(a, pltpu.VMEM) for a in kept])
        return dx, d_gates.T, dw1[None], dw3[None], dw2[None]

    return jax.shard_map(
        device_step, mesh=mesh,
        in_specs=(tok_spec, tok_spec, tok_spec, tok_spec, buf_spec, buf_spec, buf_spec, buf_spec,
                  expert_spec, expert_spec, expert_spec),
        out_specs=(tok_spec, tok_spec, buf_spec, buf_spec, buf_spec),
        check_vma=False)
```
